128 devices in a mesh: dp: 4 (over x_lo, core), ctx: 32 (over z, y, x_hi).
Axes of the slice: x: 4 (x_hi: 2, x_lo: 2; x = x_hi * 2 + x_lo), y: 4, z: 4, core: 2. Of those that a mesh axis runs over, the one named last changes fastest.
Arguments:
- queries: bfloat16 [16384, 4096], P(('dp', 'ctx')), may hold values from -6 to 6
- key_proj: bfloat16 [16384, 512], P(('dp', 'ctx')), may hold values from -6 to 6
- value_proj: bfloat16 [16384, 512], P(('dp', 'ctx')), may hold values from -6 to 6
- out_grad: bfloat16 [16384, 4096], P(('dp', 'ctx')), may hold values from -6 to 6
- row_plan: int32 [16384], P(('dp', 'ctx')), may hold values from 0 to 127, as said below
- segments: int32 [4, 4096], P('dp', 'ctx'), may hold values from 0 to 5, as said below
Outputs:
- attended: bfloat16 [16384, 4096], P(('dp', 'ctx'))
- query_grad: bfloat16 [16384, 4096], P(('dp', 'ctx'))
- key_grad: bfloat16 [16384, 512], P(('dp', 'ctx'))
- value_grad: bfloat16 [16384, 512], P(('dp', 'ctx'))
The draws below stay inside these ranges and needn't reach their ends.
Inputs may be any that keep to these rules, and one draw needn't show every extreme that they name: `row_plan`: each aligned block of 128 entries (the rows of one device) is a permutation of 0 to 127. `segments`: along each row the ids never fall, and every id from 0 to 5 occurs. Every document has at most 2176 positions, and in each row one document has exactly that many.
All inputs are finite; a program needn't handle non-finite values.
Results may differ from the reference program's by a relative error of at most 0.0083.
Values may be sent and summed in bfloat16 or wider, within the bound.
No kernel may reach another device: no remote copies, remote signals or barrier semaphores. Data moves between devices by JAX's collectives and lax.ppermute only.
A program may use at most 128 MiB of HBM per device.

```python
import jax
import jax.numpy as jnp
from jax import lax

HEADS = 32
KV_HEADS = 4
HEAD_DIM = 128
TOK_DEV = 128
DOCS = 6
SPAN_DEV = 17
SEQ = 4096
TOKENS = 16384
N_DP = 4
N_CTX = 32


def plan_table(key):
    folded = jax.random.fold_in(key, 101)
    ranks = jax.random.randint(folded, (N_DP * N_CTX, TOK_DEV), 0, 1024, dtype=jnp.int32)
    ranks = ranks * TOK_DEV + jnp.arange(TOK_DEV, dtype=jnp.int32)[None, :]
    return jnp.argsort(ranks, axis=1).astype(jnp.int32)


def segment_table(key):
    folded = jax.random.fold_in(key, 202)
    streams = jax.random.split(folded, 2)
    longest = SPAN_DEV * TOK_DEV
    others = DOCS - 1
    rest = SEQ - longest
    even_len = rest // others
    base = even_len + (jnp.arange(others, dtype=jnp.int32) < rest % others).astype(jnp.int32)
    pairs = others // 2
    upper = max(min(even_len - 1, longest - even_len - 1), 1)
    lengths = jnp.broadcast_to(base[None, :], (N_DP, others)).astype(jnp.int32)
    if pairs > 0:
        moves = jax.random.randint(streams[0], (N_DP, pairs), 0, upper, dtype=jnp.int32)
        lengths = lengths.at[:, 0:2 * pairs:2].add(moves)
        lengths = lengths.at[:, 1:2 * pairs:2].add(-moves)
    lengths = jnp.concatenate([jnp.full((N_DP, 1), longest, jnp.int32), lengths], axis=1)
    turns = jax.random.randint(streams[1], (N_DP, 1), 0, DOCS, dtype=jnp.int32)
    order = (jnp.arange(DOCS, dtype=jnp.int32)[None, :] - turns) % DOCS
    lengths = jnp.take_along_axis(lengths, order, axis=1)
    cut_points = jnp.cumsum(lengths, axis=1)[:, :DOCS - 1].astype(jnp.int32)
    positions = jnp.arange(SEQ, dtype=jnp.int32)
    return jnp.sum((positions[None, :, None] >= cut_points[:, None, :]).astype(jnp.int32), axis=2).astype(jnp.int32)


def unpack_loader(packed, plan_rows):
    columns = packed.shape[2]
    share = TOK_DEV // N_DP
    slots = jnp.transpose(packed.reshape(N_DP, N_CTX, N_DP, share, columns), (2, 1, 0, 3, 4))
    slots = slots.reshape(N_DP * N_CTX * TOK_DEV, columns)
    starts = (jnp.arange(N_DP * N_CTX, dtype=jnp.int32) * TOK_DEV)[:, None]
    target = (starts + plan_rows).reshape(-1)
    return jnp.zeros_like(slots).at[target].set(slots)


def attention_pair(key):
    folded = jax.random.fold_in(key, 303)
    streams = jax.random.split(folded, 4)
    q_dims = (N_DP, SEQ, HEADS, HEAD_DIM)
    k_dims = (N_DP, SEQ, KV_HEADS, HEAD_DIM)
    q_vals = jax.random.normal(streams[1], q_dims)
    k_vals = jax.random.normal(streams[3], k_dims)
    q_vals = jnp.clip(q_vals, -6.0, 6.0).reshape(N_DP, SEQ, HEADS * HEAD_DIM)
    k_vals = jnp.clip(k_vals, -6.0, 6.0).reshape(N_DP, SEQ, KV_HEADS * HEAD_DIM)
    plan_rows = plan_table(key)
    return (unpack_loader(q_vals, plan_rows), unpack_loader(k_vals, plan_rows))


def draw_queries(key, part):
    return attention_pair(key)[0].astype(jnp.bfloat16)


def draw_key_proj(key, part):
    return attention_pair(key)[1].astype(jnp.bfloat16)


def draw_row_plan(key, part):
    return plan_table(key).reshape(-1)


def draw_segments(key, part):
    return segment_table(key)


def block_levels(own_key, dims, cuts, smallest, largest):
    loudness, own = 1.0, jax.random.fold_in(own_key, 6)
    for dim, parts in cuts:
        heights = jnp.exp(jax.random.uniform(jax.random.fold_in(own, dim), (parts,), jnp.float32, smallest / len(cuts), largest / len(cuts)))
        loudness = loudness * jnp.repeat(heights, dims[dim] // parts).reshape([-1 if axis == dim else 1 for axis in range(len(dims))])
    return loudness


def centred(stream_key, dims, scale, bound, cuts=(), kind=jnp.bfloat16):
    entries = scale * jax.random.normal(stream_key, dims, jnp.float32)
    if cuts:
        entries = entries * block_levels(stream_key, dims, cuts, -0.22, 0.18)
    return jnp.clip(entries, -bound, bound).astype(kind)


def setup_inputs(seed: int = 0) -> dict:
    streams_of = jax.random.split(jax.random.key(seed), 7)
    return {
        "queries": draw_queries(jax.random.fold_in(streams_of[6], 71), 0),
        "key_proj": draw_key_proj(jax.random.fold_in(streams_of[6], 71), 0),
        "value_proj": centred(streams_of[2], (TOKENS, KV_HEADS * HEAD_DIM), 1.0, 6.0, ((0, 128),)),
        "out_grad": centred(streams_of[3], (TOKENS, HEADS * HEAD_DIM), 1.0, 6.0, ((0, 128),)),
        "row_plan": draw_row_plan(jax.random.fold_in(streams_of[6], 71), 0),
        "segments": draw_segments(jax.random.fold_in(streams_of[6], 71), 0),
    }


NEG = -1.0e30


def slot_index(row_plan):
    starts = (jnp.arange(N_DP * N_CTX, dtype=jnp.int32) * TOK_DEV)[:, None]
    return (starts + row_plan.reshape(N_DP * N_CTX, TOK_DEV)).reshape(-1)


def pack_rows(loader_rows, row_plan):
    columns = loader_rows.shape[1]
    share = TOK_DEV // N_DP
    picked = loader_rows[slot_index(row_plan)]
    picked = picked.reshape(N_DP, N_CTX, N_DP, share, columns)
    return jnp.transpose(picked, (2, 1, 0, 3, 4)).reshape(N_DP, SEQ, columns)


def unpack_rows(packed, row_plan):
    columns = packed.shape[2]
    share = TOK_DEV // N_DP
    slots = jnp.transpose(packed.reshape(N_DP, N_CTX, N_DP, share, columns), (2, 1, 0, 3, 4))
    slots = slots.reshape(TOKENS, columns)
    return jnp.zeros_like(slots).at[slot_index(row_plan)].set(slots)


def group_attention(inputs):
    q_flat, k_flat, v_flat, d_flat, seg_all = inputs
    seq_len = q_flat.shape[0]
    groups = HEADS // KV_HEADS
    scaling = HEAD_DIM ** -0.5
    block_len = min(256, seq_len)
    blocks = seq_len // block_len
    keys_all = k_flat.reshape(seq_len, KV_HEADS, HEAD_DIM).astype(jnp.float32)
    vals_all = v_flat.reshape(seq_len, KV_HEADS, HEAD_DIM).astype(jnp.float32)
    positions = jnp.arange(seq_len, dtype=jnp.int32)

    def block_step(running, block_idx):
        k_total, v_total = running
        offset = (block_idx * block_len).astype(jnp.int32)
        q_heads = lax.dynamic_slice_in_dim(q_flat, offset, block_len, 0).reshape(block_len, KV_HEADS, groups, HEAD_DIM).astype(jnp.float32)
        d_heads = lax.dynamic_slice_in_dim(d_flat, offset, block_len, 0).reshape(block_len, KV_HEADS, groups, HEAD_DIM).astype(jnp.float32)
        seg_rows = lax.dynamic_slice_in_dim(seg_all, offset, block_len, 0)
        pos_rows = offset + jnp.arange(block_len, dtype=jnp.int32)
        raw_scores = jnp.einsum("qkgd,skd->kgqs", q_heads, keys_all) * scaling
        visible = (seg_all[None, :] == seg_rows[:, None]) & (positions[None, :] <= pos_rows[:, None])
        scores = jnp.where(visible, raw_scores, NEG)
        row_top = jnp.max(scores, axis=3)
        row_sum = jnp.sum(jnp.where(visible, jnp.exp(scores - row_top[..., None]), 0.0), axis=3)
        log_sum = row_top + jnp.log(row_sum)
        probs = jnp.where(visible, jnp.exp(scores - log_sum[..., None]), 0.0)
        weights = lax.optimization_barrier(probs.astype(jnp.bfloat16)).astype(jnp.float32)
        out = jnp.einsum("kgqs,skd->qkgd", weights, vals_all)
        row_dot = jnp.transpose(jnp.sum(d_heads * out, axis=3), (1, 2, 0))
        dprobs = jnp.einsum("qkgd,skd->kgqs", d_heads, vals_all)
        dscore = probs * (dprobs - row_dot[..., None]) * scaling
        dscore = lax.optimization_barrier(dscore.astype(jnp.bfloat16)).astype(jnp.float32)
        q_grad = jnp.einsum("kgqs,skd->qkgd", dscore, keys_all)
        k_total = k_total + jnp.einsum("kgqs,qkgd->skd", dscore, q_heads)
        v_total = v_total + jnp.einsum("kgqs,qkgd->skd", weights, d_heads)
        emitted = (out.astype(jnp.bfloat16).reshape(block_len, -1), q_grad.astype(jnp.bfloat16).reshape(block_len, -1))
        return (k_total, v_total), emitted

    zeros = jnp.zeros((seq_len, KV_HEADS, HEAD_DIM), jnp.float32)
    (k_total, v_total), (outs, q_grads) = lax.scan(block_step, (zeros, zeros), jnp.arange(blocks, dtype=jnp.int32))
    return (outs.reshape(seq_len, -1), q_grads.reshape(seq_len, -1),
            k_total.astype(jnp.bfloat16).reshape(seq_len, -1), v_total.astype(jnp.bfloat16).reshape(seq_len, -1))


def reference(queries, key_proj, value_proj, out_grad, row_plan, segments):
    packed = (pack_rows(queries, row_plan), pack_rows(key_proj, row_plan), pack_rows(value_proj, row_plan),
              pack_rows(out_grad, row_plan), segments)
    attended, q_grad, k_grad, v_grad = lax.map(group_attention, packed)
    return (unpack_rows(attended, row_plan), unpack_rows(q_grad, row_plan),
            unpack_rows(k_grad, row_plan), unpack_rows(v_grad, row_plan))
```

```python
import functools

import jax
import jax.numpy as jnp
from jax import lax
from jax.experimental import pallas as pl
from jax.experimental.pallas import tpu as pltpu
from jax.sharding import PartitionSpec as P

HEADS = 32
KV_HEADS = 4
HEAD_DIM = 128
GROUPS = HEADS // KV_HEADS
DOCS = 6
NEG = -1e30
LOG2E = 1.4426950408889634
SHARE = 32
TOK = 128
SEQ = 4096
TQ = 256
TK = 512

IN_ROWS = 4 * SHARE + 8
OUT_ROWS = 4 * SHARE


def dot(a, b):
    return jnp.dot(a, b, preferred_element_type=jnp.float32)


def plan_matrix(plan_ref):
    rows = lax.broadcasted_iota(jnp.int32, (TOK, TOK), 0)
    return jnp.where(rows == plan_ref[...], 1.0, 0.0).astype(jnp.float32)


def pack_kernel(plan_ref, seg_ref, q_ref, d_ref, k_ref, v_ref, o_ref):
    pick = plan_matrix(plan_ref).T.astype(jnp.bfloat16)
    seg_rows = jnp.broadcast_to(seg_ref[...].astype(jnp.float32), (8, TOK)).astype(jnp.bfloat16)
    k_rows = dot(pick, k_ref[...]).astype(jnp.bfloat16)
    v_rows = dot(pick, v_ref[...]).astype(jnp.bfloat16)
    for pair in range(GROUPS // 2):
        at = slice(pair * 256, pair * 256 + 256)
        q_rows = dot(pick, q_ref[:, at]).astype(jnp.bfloat16)
        d_rows = dot(pick, d_ref[:, at]).astype(jnp.bfloat16)
        for core in range(2):
            cols = slice(core * HEAD_DIM, core * HEAD_DIM + HEAD_DIM)
            for b in range(4):
                rows = slice(b * SHARE, b * SHARE + SHARE)
                to = (b // 2, core, b % 2, pair)
                o_ref[to + (slice(0, 32),)] = q_rows[rows, cols]
                o_ref[to + (slice(32, 64),)] = d_rows[rows, cols]
                o_ref[to + (slice(64, 96),)] = k_rows[rows, :]
                o_ref[to + (slice(96, 128),)] = v_rows[rows, :]
                o_ref[to + (slice(128, 136),)] = seg_rows


def pack(queries, key_proj, value_proj, out_grad, row_plan, segments):
    wide = GROUPS * HEAD_DIM
    return pl.pallas_call(
        pack_kernel,
        grid=(KV_HEADS,),
        in_specs=[
            pl.BlockSpec((1, TOK), lambda g: (0, 0)),
            pl.BlockSpec((1, TOK), lambda g: (0, 0)),
            pl.BlockSpec((TOK, wide), lambda g: (0, g)),
            pl.BlockSpec((TOK, wide), lambda g: (0, g)),
            pl.BlockSpec((TOK, HEAD_DIM), lambda g: (0, g)),
            pl.BlockSpec((TOK, HEAD_DIM), lambda g: (0, g)),
        ],
        out_specs=pl.BlockSpec(
            (2, 2, 2, GROUPS // 2, IN_ROWS, HEAD_DIM), lambda g: (0, 0, 0, g, 0, 0)
        ),
        out_shape=jax.ShapeDtypeStruct((2, 2, 2, 16, IN_ROWS, HEAD_DIM), jnp.bfloat16),
        name="pack",
    )(row_plan.reshape(1, TOK), segments, queries, out_grad, key_proj, value_proj)


def unpack_kernel(plan_ref, y_ref, att_ref, qg_ref, kg_ref, vg_ref):
    put = plan_matrix(plan_ref).astype(jnp.bfloat16)

    def slots(core, pair, first):
        parts = [
            y_ref[b // 2, core, b % 2, pair, slice(first, first + SHARE)] for b in range(4)
        ]
        return jnp.concatenate(parts, axis=0)

    k_sum = jnp.zeros((TOK, HEAD_DIM), jnp.float32)
    v_sum = jnp.zeros((TOK, HEAD_DIM), jnp.float32)
    for pair in range(GROUPS // 2):
        for core in range(2):
            at = slice((pair * 2 + core) * HEAD_DIM, (pair * 2 + core + 1) * HEAD_DIM)
            att_ref[:, at] = dot(put, slots(core, pair, 0)).astype(jnp.bfloat16)
            qg_ref[:, at] = dot(put, slots(core, pair, 32)).astype(jnp.bfloat16)
            k_sum = k_sum + slots(core, pair, 64).astype(jnp.float32)
            v_sum = v_sum + slots(core, pair, 96).astype(jnp.float32)
    kg_ref[...] = dot(put, k_sum.astype(jnp.bfloat16)).astype(jnp.bfloat16)
    vg_ref[...] = dot(put, v_sum.astype(jnp.bfloat16)).astype(jnp.bfloat16)


def unpack(back, row_plan):
    wide = GROUPS * HEAD_DIM
    return pl.pallas_call(
        unpack_kernel,
        grid=(KV_HEADS,),
        in_specs=[
            pl.BlockSpec((1, TOK), lambda g: (0, 0)),
            pl.BlockSpec(
                (2, 2, 2, GROUPS // 2, OUT_ROWS, HEAD_DIM), lambda g: (0, 0, 0, g, 0, 0)
            ),
        ],
        out_specs=[
            pl.BlockSpec((TOK, wide), lambda g: (0, g)),
            pl.BlockSpec((TOK, wide), lambda g: (0, g)),
            pl.BlockSpec((TOK, HEAD_DIM), lambda g: (0, g)),
            pl.BlockSpec((TOK, HEAD_DIM), lambda g: (0, g)),
        ],
        out_shape=[
            jax.ShapeDtypeStruct((TOK, HEADS * HEAD_DIM), jnp.bfloat16),
            jax.ShapeDtypeStruct((TOK, HEADS * HEAD_DIM), jnp.bfloat16),
            jax.ShapeDtypeStruct((TOK, KV_HEADS * HEAD_DIM), jnp.bfloat16),
            jax.ShapeDtypeStruct((TOK, KV_HEADS * HEAD_DIM), jnp.bfloat16),
        ],
        name="unpack",
    )(row_plan.reshape(1, TOK), back)


def attention_kernel(
    group_ref, z_ref, o_ref, q_s, d_s, k_s, v_s, qt_s, dt_s, kt_s, vt_s, s_s, dk_s, dv_s, ot_s, qg_s
):
    scaling = HEAD_DIM ** (-0.5)
    to_exp2 = scaling * LOG2E

    def lay_out(c, carry):
        at = pl.ds(pl.multiple_of(c * TOK, TOK), TOK)
        for n, (rows_s, cols_s) in enumerate(((q_s, qt_s), (d_s, dt_s), (k_s, kt_s), (v_s, vt_s))):
            tile = z_ref[:, c, n * SHARE : n * SHARE + SHARE, :].reshape(TOK, HEAD_DIM)
            rows_s[at, :] = tile
            cols_s[:, at] = tile.T
        dk_s[at, :] = jnp.zeros((TOK, HEAD_DIM), jnp.float32)
        dv_s[at, :] = jnp.zeros((TOK, HEAD_DIM), jnp.float32)
        return carry

    lax.fori_loop(0, SEQ // TOK, lay_out, 0)

    ids = z_ref[group_ref[0], :, 4 * SHARE : 4 * SHARE + 8, :].astype(jnp.float32)
    cuts = [
        (jnp.sum((ids < float(doc)).astype(jnp.float32)) * 0.125).astype(jnp.int32)
        for doc in range(1, DOCS)
    ]

    def doc_start(position):
        start = jnp.zeros_like(position)
        for cut in cuts:
            start = jnp.maximum(start, jnp.where(position >= cut, cut, 0))
        return start

    def query_tile(i, carry):
        first_row = i * TQ
        q_at = pl.ds(pl.multiple_of(first_row, TQ), TQ)
        first_key = doc_start(first_row)
        lo = first_key // TK
        hi = (first_row + TQ - 1) // TK + 1
        rows = first_row + lax.broadcasted_iota(jnp.int32, (1, TQ), 1)
        starts = doc_start(rows)
        qt = qt_s[:, q_at]
        dt = dt_s[:, q_at]

        def score_step(j, top):
            k_at = pl.ds(pl.multiple_of(j * TK, TK), TK)
            scores = dot(k_s[k_at, :], qt)
            keys = j * TK + lax.broadcasted_iota(jnp.int32, (TK, TQ), 0)
            visible = (keys <= rows) & (keys >= starts)
            scores = jnp.where(visible, scores, NEG)
            s_s[k_at, :] = scores
            return jnp.maximum(top, jnp.max(scores.reshape(TK // 8, 8, TQ), axis=0))

        top = lax.fori_loop(lo, hi, score_step, jnp.full((8, TQ), NEG, jnp.float32))
        top = jnp.max(top, axis=0, keepdims=True)

        def exp_step(j, total):
            k_at = pl.ds(pl.multiple_of(j * TK, TK), TK)
            part = jnp.exp2((s_s[k_at, :] - top) * to_exp2)
            s_s[k_at, :] = part
            return total + jnp.sum(part.reshape(TK // 8, 8, TQ), axis=0)

        total = lax.fori_loop(lo, hi, exp_step, jnp.zeros((8, TQ), jnp.float32))
        share = 1.0 / jnp.sum(total, axis=0, keepdims=True)

        ot_s[...] = jnp.zeros_like(ot_s)
        qg_s[...] = jnp.zeros_like(qg_s)

        def out_step(j, carry):
            k_at = pl.ds(pl.multiple_of(j * TK, TK), TK)
            weights = (s_s[k_at, :] * share).astype(jnp.bfloat16)
            ot_s[...] += dot(vt_s[:, k_at], weights)
            return carry

        lax.fori_loop(lo, hi, out_step, 0)
        out_t = ot_s[...]
        row_dot = jnp.sum(dt.astype(jnp.float32) * out_t, axis=0, keepdims=True)

        def grad_step(j, carry):
            k_at = pl.ds(pl.multiple_of(j * TK, TK), TK)
            probs = s_s[k_at, :] * share
            dprobs = dot(v_s[k_at, :], dt)
            dscore = (probs * (dprobs - row_dot) * scaling).astype(jnp.bfloat16)
            dv_s[k_at, :] += dot(probs.astype(jnp.bfloat16), d_s[q_at, :])
            dk_s[k_at, :] += dot(dscore, q_s[q_at, :])
            qg_s[...] += dot(kt_s[:, k_at], dscore)
            return carry

        lax.fori_loop(lo, hi, grad_step, 0)

        out_rows = out_t.astype(jnp.bfloat16).T
        grad_rows = qg_s[...].astype(jnp.bfloat16).T
        for n in range(TQ // TOK):
            c = i * (TQ // TOK) + n
            at = slice(n * TOK, n * TOK + TOK)
            o_ref[:, c, 0:32, :] = out_rows[at].reshape(4, SHARE, HEAD_DIM)
            o_ref[:, c, 32:64, :] = grad_rows[at].reshape(4, SHARE, HEAD_DIM)
        return carry

    lax.fori_loop(0, SEQ // TQ, query_tile, 0)

    def give_back(c, carry):
        at = pl.ds(pl.multiple_of(c * TOK, TOK), TOK)
        o_ref[:, c, 64:96, :] = dk_s[at, :].astype(jnp.bfloat16).reshape(4, SHARE, HEAD_DIM)
        o_ref[:, c, 96:128, :] = dv_s[at, :].astype(jnp.bfloat16).reshape(4, SHARE, HEAD_DIM)
        return carry

    lax.fori_loop(0, SEQ // TOK, give_back, 0)


def attention(group, z):
    tall = pltpu.VMEM((SEQ, HEAD_DIM), jnp.bfloat16)
    flat = pltpu.VMEM((HEAD_DIM, SEQ), jnp.bfloat16)
    return pl.pallas_call(
        attention_kernel,
        in_specs=[
            pl.BlockSpec(memory_space=pltpu.SMEM),
            pl.BlockSpec(memory_space=pltpu.VMEM),
        ],
        out_specs=pl.BlockSpec(memory_space=pltpu.VMEM),
        out_shape=jax.ShapeDtypeStruct((4, 32, OUT_ROWS, HEAD_DIM), jnp.bfloat16),
        scratch_shapes=[tall] * 4
        + [flat] * 4
        + [
            pltpu.VMEM((SEQ, TQ), jnp.float32),
            pltpu.VMEM((SEQ, HEAD_DIM), jnp.float32),
            pltpu.VMEM((SEQ, HEAD_DIM), jnp.float32),
            pltpu.VMEM((HEAD_DIM, TQ), jnp.float32),
            pltpu.VMEM((HEAD_DIM, TQ), jnp.float32),
        ],
        compiler_params=pltpu.CompilerParams(vmem_limit_bytes=56 << 20),
        name="attention",
    )(group, z)


def on_device(queries, key_proj, value_proj, out_grad, row_plan, segments):
    sent = pack(queries, key_proj, value_proj, out_grad, row_plan, segments)
    here = lax.all_to_all(
        sent.reshape(TOK, IN_ROWS, HEAD_DIM), ("dp", "ctx"), split_axis=0, concat_axis=0, tiled=True
    )
    group = (lax.axis_index("dp") // 2) * 2 + lax.axis_index("ctx") // 16
    done = attention(
        group.astype(jnp.int32).reshape(1), here.reshape(4, 32, IN_ROWS, HEAD_DIM)
    )
    back = lax.all_to_all(
        done.reshape(TOK, OUT_ROWS, HEAD_DIM), ("dp", "ctx"), split_axis=0, concat_axis=0, tiled=True
    )
    return tuple(unpack(back.reshape(2, 2, 2, 16, OUT_ROWS, HEAD_DIM), row_plan))


def solution(mesh):
    rows = P(("dp", "ctx"), None)
    return jax.shard_map(
        on_device,
        mesh=mesh,
        in_specs=(rows, rows, rows, rows, P(("dp", "ctx")), P("dp", "ctx")),
        out_specs=(rows, rows, rows, rows),
        check_vma=False,
    )
```

```python
import functools

import jax
import jax.numpy as jnp
from jax import lax
from jax.experimental import pallas as pl
from jax.experimental.pallas import tpu as pltpu
from jax.sharding import PartitionSpec as P

HEADS = 32
KV_HEADS = 4
HEAD_DIM = 128
GROUPS = HEADS // KV_HEADS
DOCS = 6
NEG = -1e30
LOG2E = 1.4426950408889634
SHARE = 32
TOK = 128
SEQ = 4096
TQ = 256
TK = 512

IN_ROWS = 3 * SHARE + 8
OUT_ROWS = 3 * SHARE
PIECES = 4


def dot(a, b):
    return jnp.dot(a, b, preferred_element_type=jnp.float32)


def dot_nt(a, b):
    return lax.dot_general(a, b, (((1,), (1,)), ((), ())), preferred_element_type=jnp.float32)


def plan_matrix(plan_ref):
    rows = lax.broadcasted_iota(jnp.int32, (TOK, TOK), 0)
    return jnp.where(rows == plan_ref[...], 1.0, 0.0).astype(jnp.float32)


def pack_kernel(plan_ref, seg_ref, q_ref, d_ref, k_ref, v_ref, o_ref):
    pick = plan_matrix(plan_ref).T.astype(jnp.bfloat16)
    seg_rows = jnp.broadcast_to(seg_ref[...].astype(jnp.float32), (8, TOK)).astype(jnp.bfloat16)
    k_rows = dot(pick, k_ref[...]).astype(jnp.bfloat16)
    v_rows = dot(pick, v_ref[...]).astype(jnp.bfloat16)
    for pair in range(GROUPS // 2):
        at = slice(pair * 256, pair * 256 + 256)
        q_rows = dot(pick, q_ref[:, at]).astype(jnp.bfloat16)
        d_rows = dot(pick, d_ref[:, at]).astype(jnp.bfloat16)
        for core in range(2):
            cols = slice(core * HEAD_DIM, core * HEAD_DIM + HEAD_DIM)
            for b in range(4):
                rows = slice(b * SHARE, b * SHARE + SHARE)
                to = (b // 2, core, b % 2, pair)
                o_ref[to + (slice(0, 32),)] = q_rows[rows, cols]
                o_ref[to + (slice(32, 64),)] = d_rows[rows, cols]
                o_ref[to + (slice(64, 96),)] = (k_rows, v_rows)[core][rows, :]
                o_ref[to + (slice(96, 104),)] = seg_rows


def pack(queries, key_proj, value_proj, out_grad, row_plan, segments):
    wide = GROUPS * HEAD_DIM
    return pl.pallas_call(
        pack_kernel,
        grid=(KV_HEADS,),
        in_specs=[
            pl.BlockSpec((1, TOK), lambda g: (0, 0)),
            pl.BlockSpec((1, TOK), lambda g: (0, 0)),
            pl.BlockSpec((TOK, wide), lambda g: (0, g)),
            pl.BlockSpec((TOK, wide), lambda g: (0, g)),
            pl.BlockSpec((TOK, HEAD_DIM), lambda g: (0, g)),
            pl.BlockSpec((TOK, HEAD_DIM), lambda g: (0, g)),
        ],
        out_specs=pl.BlockSpec(
            (2, 2, 2, GROUPS // 2, IN_ROWS, HEAD_DIM), lambda g: (0, 0, 0, g, 0, 0)
        ),
        out_shape=jax.ShapeDtypeStruct((2, 2, 2, 16, IN_ROWS, HEAD_DIM), jnp.bfloat16),
        name="pack",
    )(row_plan.reshape(1, TOK), segments, queries, out_grad, key_proj, value_proj)


def unpack_kernel(plan_ref, y_ref, att_ref, qg_ref, kg_ref, vg_ref):
    put = plan_matrix(plan_ref).astype(jnp.bfloat16)

    def slots(core, pair, first):
        parts = [
            y_ref[b // 2, core, b % 2, pair, slice(first, first + SHARE)] for b in range(4)
        ]
        return jnp.concatenate(parts, axis=0)

    k_sum = jnp.zeros((TOK, HEAD_DIM), jnp.float32)
    v_sum = jnp.zeros((TOK, HEAD_DIM), jnp.float32)
    for pair in range(GROUPS // 2):
        for core in range(2):
            at = slice((pair * 2 + core) * HEAD_DIM, (pair * 2 + core + 1) * HEAD_DIM)
            att_ref[:, at] = dot(put, slots(core, pair, 0)).astype(jnp.bfloat16)
            qg_ref[:, at] = dot(put, slots(core, pair, 32)).astype(jnp.bfloat16)
        k_sum = k_sum + slots(0, pair, 64).astype(jnp.float32)
        v_sum = v_sum + slots(1, pair, 64).astype(jnp.float32)
    kg_ref[...] = dot(put, k_sum.astype(jnp.bfloat16)).astype(jnp.bfloat16)
    vg_ref[...] = dot(put, v_sum.astype(jnp.bfloat16)).astype(jnp.bfloat16)


def unpack(back, row_plan):
    wide = GROUPS * HEAD_DIM
    return pl.pallas_call(
        unpack_kernel,
        grid=(KV_HEADS,),
        in_specs=[
            pl.BlockSpec((1, TOK), lambda g: (0, 0)),
            pl.BlockSpec(
                (2, 2, 2, GROUPS // 2, OUT_ROWS, HEAD_DIM), lambda g: (0, 0, 0, g, 0, 0)
            ),
        ],
        out_specs=[
            pl.BlockSpec((TOK, wide), lambda g: (0, g)),
            pl.BlockSpec((TOK, wide), lambda g: (0, g)),
            pl.BlockSpec((TOK, HEAD_DIM), lambda g: (0, g)),
            pl.BlockSpec((TOK, HEAD_DIM), lambda g: (0, g)),
        ],
        out_shape=[
            jax.ShapeDtypeStruct((TOK, HEADS * HEAD_DIM), jnp.bfloat16),
            jax.ShapeDtypeStruct((TOK, HEADS * HEAD_DIM), jnp.bfloat16),
            jax.ShapeDtypeStruct((TOK, KV_HEADS * HEAD_DIM), jnp.bfloat16),
            jax.ShapeDtypeStruct((TOK, KV_HEADS * HEAD_DIM), jnp.bfloat16),
        ],
        name="unpack",
    )(row_plan.reshape(1, TOK), back)


def attention_kernel(
    z_ref,
    other_ref,
    o_ref,
    keep_ref,
    give_ref,
    qd_b,
    kv_b,
    seg_b,
    o_b,
    q_s,
    qa_s,
    d_s,
    k_s,
    ka_s,
    v_s,
    dt_s,
    kt_s,
    vt_s,
    p_even,
    p_odd,
    tops_even,
    tops_odd,
    rows_even,
    rows_odd,
    dk_s,
    dv_s,
    ot_s,
    qg_s,
    top_s,
    sum_s,
    in_sem,
    seg_sem,
    out_sem,
    keep_sem,
    give_sem,
):
    scaling = HEAD_DIM ** (-0.5)
    to_exp2 = scaling * LOG2E
    tall = (TK // 8, 8, TQ)
    core = lax.axis_index("dp") % 2
    group = (lax.axis_index("dp") // 2) * 2 + lax.axis_index("ctx") // 16
    per_piece = SEQ // TOK // PIECES

    def piece(n):
        at = pl.ds(n * per_piece, per_piece)
        return (
            pltpu.make_async_copy(z_ref.at[:, at, 0:64], qd_b.at[:, at], in_sem.at[n, 0]),
            pltpu.make_async_copy(z_ref.at[:, at, 64:96], kv_b.at[core, :, at], in_sem.at[n, 1]),
            pltpu.make_async_copy(other_ref.at[:, at], kv_b.at[1 - core, :, at], in_sem.at[n, 2]),
        )

    seg_copy = pltpu.make_async_copy(z_ref.at[group, :, 96:104], seg_b, seg_sem)
    seg_copy.start()
    pieces = [piece(n) for n in range(PIECES)]
    for copies in pieces:
        for copy in copies:
            copy.start()
    seg_copy.wait()

    ids = seg_b[...].astype(jnp.float32)
    cuts = [
        (jnp.sum((ids < float(doc)).astype(jnp.float32)) * 0.125).astype(jnp.int32)
        for doc in range(1, DOCS)
    ]

    lane = lax.broadcasted_iota(jnp.int32, (1, HEAD_DIM), 1)
    ends = jnp.zeros((1, HEAD_DIM), jnp.int32)
    for n, cut in enumerate(cuts):
        ends = jnp.where(lane == n, cut, ends)
    used = lane < DOCS - 1

    def lay_out(c, carry):
        at = pl.ds(pl.multiple_of(c * TOK, TOK), TOK)
        key_tile = kv_b[0, :, c].reshape(TOK, HEAD_DIM)
        value_tile = kv_b[1, :, c].reshape(TOK, HEAD_DIM)
        d_tile = qd_b[:, c, SHARE : 2 * SHARE, :].reshape(TOK, HEAD_DIM)
        q_s[at, :] = qd_b[:, c, 0:SHARE, :].reshape(TOK, HEAD_DIM)
        k_s[at, :] = key_tile
        v_s[at, :] = value_tile
        d_s[at, :] = d_tile
        kt_s[c] = key_tile.T
        vt_s[c] = value_tile.T
        dt_s[c] = d_tile.T
        spot = c * TOK + lax.broadcasted_iota(jnp.int32, (TOK, HEAD_DIM), 0)
        early = spot < ends
        qa_s[at, :] = jnp.where(used & ~early, NEG, 0.0).astype(jnp.bfloat16)
        ka_s[at, :] = jnp.where(used & early, 1.0, 0.0).astype(jnp.bfloat16)
        dk_s[at, :] = jnp.zeros((TOK, HEAD_DIM), jnp.float32)
        dv_s[at, :] = jnp.zeros((TOK, HEAD_DIM), jnp.float32)
        return carry

    for n in range(PIECES):
        for copy in pieces[n]:
            copy.wait()
        lax.fori_loop(n * per_piece, (n + 1) * per_piece, lay_out, 0, unroll=2)

    def doc_start(position):
        start = jnp.zeros_like(position)
        for cut in cuts:
            start = jnp.maximum(start, jnp.where(position >= cut, cut, 0))
        return start

    def chunks(i):
        first_row = i * TQ
        return doc_start(first_row) // TK, (first_row + TQ - 1) // TK + 1

    def key_at(j):
        return pl.ds(pl.multiple_of(j * TK, TK), TK)

    def query_at(i):
        return pl.ds(pl.multiple_of(i * TQ, TQ), TQ)

    def send_rows(i, n):
        at = pl.ds(i * (TQ // TOK), TQ // TOK)
        rows = slice(n * SHARE, n * SHARE + SHARE)
        return pltpu.make_async_copy(o_b.at[n, :, at], o_ref.at[:, at, rows], out_sem.at[n])

    def side_by_side(cols_s, first, count):
        return jnp.concatenate([cols_s[first + n] for n in range(count)], axis=1)

    def clear_forward():
        top_s[...] = jnp.full((8, TQ), NEG, jnp.float32)
        sum_s[...] = jnp.zeros((8, TQ), jnp.float32)
        ot_s[...] = jnp.zeros((HEAD_DIM, TQ), jnp.float32)

    def scores_of(i, j, p_s):
        k_at, q_at = key_at(j), query_at(i)
        keys = jnp.concatenate([k_s[k_at, :], ka_s[k_at, :]], axis=1)
        scores = dot_nt(keys, jnp.concatenate([q_s[q_at, :], qa_s[q_at, :]], axis=1))
        rows = i * TQ - j * TK + lax.broadcasted_iota(jnp.int32, (1, TQ), 1)
        keys = lax.broadcasted_iota(jnp.int32, (TK, TQ), 0)
        return jnp.where(keys <= rows, scores, NEG).reshape(tall)

    def soften(scores, j, p_s, tops_s):
        before = top_s[...]
        here = jnp.max(jnp.max(scores, axis=0), axis=0, keepdims=True)
        top = jnp.maximum(before, jnp.broadcast_to(here, (8, TQ)))
        part = jnp.exp2((scores - top) * to_exp2)
        fade = jnp.exp2((before - top) * to_exp2)
        sum_s[...] = sum_s[...] * fade + jnp.sum(part, axis=0)
        top_s[...] = top
        tops_s[j] = top
        part = part.reshape(TK, TQ)
        p_s[key_at(j), :] = part
        return part.astype(jnp.bfloat16), fade

    def add_out(j, part, fade):
        faded = (ot_s[...].reshape(HEAD_DIM // 8, 8, TQ) * fade).reshape(HEAD_DIM, TQ)
        ot_s[...] = faded + dot(side_by_side(vt_s, j * (TK // TOK), TK // TOK), part)

    def forward_step(i, j, p_s, tops_s):
        part, fade = soften(scores_of(i, j, p_s), j, p_s, tops_s)
        add_out(j, part, fade)

    def both_steps(i, j, p_s, tops_s, i_now, j_now, p_now, tops_now, rows_now):
        scores = scores_of(i, j, p_s)
        k_at, q_at = key_at(j_now), query_at(i_now)
        dprobs = dot_nt(v_s[k_at, :], d_s[q_at, :]).reshape(tall)
        share = jnp.exp2((tops_now[j_now] - rows_now[0]) * to_exp2) * rows_now[1]
        held = p_now[k_at, :].reshape(tall)
        weights = (held * share).reshape(TK, TQ).astype(jnp.bfloat16)
        dv_s[k_at, :] += dot(weights, d_s[q_at, :])
        part, fade = soften(scores, j, p_s, tops_s)
        dscore = (held * (share * scaling)) * (dprobs - rows_now[2])
        dscore = dscore.reshape(TK, TQ).astype(jnp.bfloat16)
        dk_s[k_at, :] += dot(dscore, q_s[q_at, :])
        qg_s[...] += dot(side_by_side(kt_s, j_now * (TK // TOK), TK // TOK), dscore)
        add_out(j, part, fade)

    def forward_end(i, rows_s):
        share = 1.0 / jnp.sum(sum_s[...], axis=0, keepdims=True)
        out_t = ot_s[...] * share
        dt = side_by_side(dt_s, i * (TQ // TOK), TQ // TOK)
        row_dot = jnp.sum(dt.astype(jnp.float32) * out_t, axis=0, keepdims=True)
        rows_s[0] = top_s[...]
        rows_s[1] = jnp.broadcast_to(share, (8, TQ))
        rows_s[2] = jnp.broadcast_to(row_dot, (8, TQ))
        out_rows = out_t.astype(jnp.bfloat16).T
        for n in range(TQ // TOK):
            tile = out_rows[n * TOK : n * TOK + TOK].reshape(4, SHARE, HEAD_DIM)
            o_b[0, :, i * (TQ // TOK) + n] = tile
        send_rows(i, 0).start()
        clear_forward()

    def gradient_step(i, j, p_s, tops_s, rows_s):
        k_at, q_at = key_at(j), query_at(i)
        share = jnp.exp2((tops_s[j] - rows_s[0]) * to_exp2) * rows_s[1]
        dprobs = dot_nt(v_s[k_at, :], d_s[q_at, :]).reshape(tall)
        part = p_s[k_at, :].reshape(tall)
        weights = (part * share).reshape(TK, TQ).astype(jnp.bfloat16)
        dv_s[k_at, :] += dot(weights, d_s[q_at, :])
        dscore = (part * (share * scaling)) * (dprobs - rows_s[2])
        dscore = dscore.reshape(TK, TQ).astype(jnp.bfloat16)
        dk_s[k_at, :] += dot(dscore, q_s[q_at, :])
        qg_s[...] += dot(side_by_side(kt_s, j * (TK // TOK), TK // TOK), dscore)

    def gradient_end(i):
        grad_rows = qg_s[...].astype(jnp.bfloat16).T
        for n in range(TQ // TOK):
            tile = grad_rows[n * TOK : n * TOK + TOK].reshape(4, SHARE, HEAD_DIM)
            o_b[1, :, i * (TQ // TOK) + n] = tile
        send_rows(i, 1).start()
        qg_s[...] = jnp.zeros((HEAD_DIM, TQ), jnp.float32)

    even = (p_even, tops_even, rows_even)
    odd = (p_odd, tops_odd, rows_odd)

    def stage(i_next, ahead, i_now, behind):
        now_lo, now_hi = chunks(i_now)
        next_lo, next_hi = chunks(jnp.minimum(i_next, SEQ // TQ - 1))
        next_n = jnp.where(i_next < SEQ // TQ, next_hi - next_lo, 0)
        now_n = now_hi - now_lo
        both = jnp.minimum(next_n, now_n)

        def together(t, carry):
            both_steps(i_next, next_lo + t, *ahead[:2], i_now, now_lo + t, *behind)
            return carry

        def ahead_only(t, carry):
            forward_step(i_next, next_lo + t, *ahead[:2])
            return carry

        def behind_only(t, carry):
            gradient_step(i_now, now_lo + t, *behind)
            return carry

        lax.fori_loop(0, both, together, 0)
        lax.fori_loop(both, next_n, ahead_only, 0)
        lax.fori_loop(both, now_n, behind_only, 0)

        @pl.when(i_next < SEQ // TQ)
        def _():
            forward_end(i_next, ahead[2])

        gradient_end(i_now)

    clear_forward()
    qg_s[...] = jnp.zeros((HEAD_DIM, TQ), jnp.float32)
    forward_step(0, 0, *even[:2])
    forward_end(0, rows_even)

    def two_stages(m, carry):
        stage(2 * m + 1, odd, 2 * m, even)
        stage(2 * m + 2, even, 2 * m + 1, odd)
        return carry

    lax.fori_loop(0, SEQ // TQ // 2, two_stages, 0)

    def give_back(c, carry):
        at = pl.ds(pl.multiple_of(c * TOK, TOK), TOK)
        kv_b[0, :, c] = dk_s[at, :].astype(jnp.bfloat16).reshape(4, SHARE, HEAD_DIM)
        kv_b[1, :, c] = dv_s[at, :].astype(jnp.bfloat16).reshape(4, SHARE, HEAD_DIM)
        return carry

    lax.fori_loop(0, SEQ // TOK, give_back, 0, unroll=2)
    keep_copy = pltpu.make_async_copy(kv_b.at[core], keep_ref, keep_sem)
    give_copy = pltpu.make_async_copy(kv_b.at[1 - core], give_ref, give_sem)
    keep_copy.start()
    give_copy.start()
    for n in range(2):
        rows = slice(n * SHARE, n * SHARE + SHARE)
        pltpu.make_async_copy(o_b.at[n], o_ref.at[:, :, rows], out_sem.at[n]).wait()
    keep_copy.wait()
    give_copy.wait()


def attention(z, other):
    tall = pltpu.VMEM((SEQ, HEAD_DIM), jnp.bfloat16)
    flat = pltpu.VMEM((SEQ // TOK, TOK, HEAD_DIM), jnp.bfloat16)
    anywhere = pl.BlockSpec(memory_space=pltpu.HBM)
    part = jax.ShapeDtypeStruct((4, 32, SHARE, HEAD_DIM), jnp.bfloat16)
    return pl.pallas_call(
        attention_kernel,
        in_specs=[anywhere, anywhere],
        out_specs=[anywhere, anywhere, anywhere],
        out_shape=[jax.ShapeDtypeStruct((4, 32, OUT_ROWS, HEAD_DIM), jnp.bfloat16), part, part],
        scratch_shapes=[
            pltpu.VMEM((4, 32, 2 * SHARE, HEAD_DIM), jnp.bfloat16),
            pltpu.VMEM((2, 4, 32, SHARE, HEAD_DIM), jnp.bfloat16),
            pltpu.VMEM((32, 8, HEAD_DIM), jnp.bfloat16),
            pltpu.VMEM((2, 4, 32, SHARE, HEAD_DIM), jnp.bfloat16),
        ]
        + [tall] * 6
        + [flat] * 3
        + [pltpu.VMEM((SEQ, TQ), jnp.float32)] * 2
        + [pltpu.VMEM((SEQ // TK, 8, TQ), jnp.float32)] * 2
        + [pltpu.VMEM((3, 8, TQ), jnp.float32)] * 2
        + [pltpu.VMEM((SEQ, HEAD_DIM), jnp.float32)] * 2
        + [pltpu.VMEM((HEAD_DIM, TQ), jnp.float32)] * 2
        + [pltpu.VMEM((8, TQ), jnp.float32)] * 2
        + [
            pltpu.SemaphoreType.DMA((PIECES, 3)),
            pltpu.SemaphoreType.DMA,
            pltpu.SemaphoreType.DMA((2,)),
            pltpu.SemaphoreType.DMA,
            pltpu.SemaphoreType.DMA,
        ],
        compiler_params=pltpu.CompilerParams(vmem_limit_bytes=56 << 20),
        name="attention",
    )(z, other)


def join_kernel(o_ref, keep_ref, got_ref, out_ref):
    both = keep_ref[...].astype(jnp.float32) + got_ref[...].astype(jnp.float32)
    out_ref[...] = both.astype(jnp.bfloat16)


def join(rows, keep, got):
    part = pl.BlockSpec((4, 8, SHARE, HEAD_DIM), lambda c: (0, c, 0, 0))
    return pl.pallas_call(
        join_kernel,
        grid=(4,),
        in_specs=[pl.BlockSpec(memory_space=pltpu.HBM), part, part],
        out_specs=pl.BlockSpec((4, 8, SHARE, HEAD_DIM), lambda c: (0, c, 2, 0)),
        out_shape=jax.ShapeDtypeStruct(rows.shape, rows.dtype),
        input_output_aliases={0: 0},
        name="join",
    )(rows, keep, got)


def to_other_core(x):
    return lax.ppermute(x, "dp", [(0, 1), (1, 0), (2, 3), (3, 2)])


def on_device(queries, key_proj, value_proj, out_grad, row_plan, segments):
    sent = pack(queries, key_proj, value_proj, out_grad, row_plan, segments)
    here = lax.all_to_all(
        sent.reshape(TOK, IN_ROWS, HEAD_DIM), ("dp", "ctx"), split_axis=0, concat_axis=0, tiled=True
    ).reshape(4, 32, IN_ROWS, HEAD_DIM)
    other = to_other_core(here[:, :, 64:96, :])
    rows, keep, give = attention(here, other)
    done = join(rows, keep, to_other_core(give))
    back = lax.all_to_all(
        done.reshape(TOK, OUT_ROWS, HEAD_DIM), ("dp", "ctx"), split_axis=0, concat_axis=0, tiled=True
    )
    return tuple(unpack(back.reshape(2, 2, 2, 16, OUT_ROWS, HEAD_DIM), row_plan))


def solution(mesh):
    rows = P(("dp", "ctx"), None)
    return jax.shard_map(
        on_device,
        mesh=mesh,
        in_specs=(rows, rows, rows, rows, P(("dp", "ctx")), P("dp", "ctx")),
        out_specs=(rows, rows, rows, rows),
        check_vma=False,
    )
```

```python
import functools

import jax
import jax.numpy as jnp
from jax import lax
from jax.experimental import pallas as pl
from jax.experimental.pallas import tpu as pltpu
from jax.sharding import PartitionSpec as P

HEADS = 32
KV_HEADS = 4
HEAD_DIM = 128
GROUPS = HEADS // KV_HEADS
DOCS = 6
NEG = -1e30
LOG2E = 1.4426950408889634
SHARE = 32
TOK = 128
SEQ = 4096
TQ = 256
TK = 512

IN_ROWS = 3 * SHARE + 8
OUT_ROWS = 3 * SHARE


def dot(a, b):
    return jnp.dot(a, b, preferred_element_type=jnp.float32)


def dot_nt(a, b):
    return lax.dot_general(a, b, (((1,), (1,)), ((), ())), preferred_element_type=jnp.float32)


def plan_matrix(plan_ref):
    rows = lax.broadcasted_iota(jnp.int32, (TOK, TOK), 0)
    return jnp.where(rows == plan_ref[...], 1.0, 0.0).astype(jnp.float32)


def pack_kernel(
    plan_hbm,
    seg_hbm,
    q_hbm,
    d_hbm,
    k_hbm,
    v_hbm,
    o_ref,
    plan_ref,
    seg_ref,
    q_ref,
    d_ref,
    k_ref,
    v_ref,
    sems,
):
    small = [
        pltpu.make_async_copy(plan_hbm, plan_ref, sems.at[0]),
        pltpu.make_async_copy(k_hbm, k_ref, sems.at[1]),
        pltpu.make_async_copy(v_hbm, v_ref, sems.at[2]),
        pltpu.make_async_copy(seg_hbm, seg_ref, sems.at[3]),
    ]
    for copy in small:
        copy.start()
    large = []
    for g in range(KV_HEADS):
        at = pl.ds(g * GROUPS * HEAD_DIM, GROUPS * HEAD_DIM)
        large.append(
            (
                pltpu.make_async_copy(q_hbm.at[:, at], q_ref.at[:, at], sems.at[4 + 2 * g]),
                pltpu.make_async_copy(d_hbm.at[:, at], d_ref.at[:, at], sems.at[5 + 2 * g]),
            )
        )
        for copy in large[g]:
            copy.start()
    for copy in small:
        copy.wait()
    pick = plan_matrix(plan_ref).T.astype(jnp.bfloat16)
    seg_rows = jnp.broadcast_to(seg_ref[...].astype(jnp.float32), (8, TOK)).astype(jnp.bfloat16)
    for g in range(KV_HEADS):
        cols = slice(g * HEAD_DIM, g * HEAD_DIM + HEAD_DIM)
        k_rows = dot(pick, k_ref[:, cols]).astype(jnp.bfloat16)
        v_rows = dot(pick, v_ref[:, cols]).astype(jnp.bfloat16)
        for pair in range(GROUPS // 2):
            for core in range(2):
                for b in range(4):
                    rows = slice(b * SHARE, b * SHARE + SHARE)
                    o_ref[b // 2, core, b % 2, g * (GROUPS // 2) + pair, 64:96] = (k_rows, v_rows)[
                        core
                    ][rows]
                    o_ref[b // 2, core, b % 2, g * (GROUPS // 2) + pair, 96:104] = seg_rows
        for n, (copy, ref) in enumerate(zip(large[g], (q_ref, d_ref))):
            copy.wait()
            for pair in range(GROUPS // 2):
                first = (g * (GROUPS // 2) + pair) * 2 * HEAD_DIM
                both = dot(pick, ref[:, first : first + 2 * HEAD_DIM]).astype(jnp.bfloat16)
                for core in range(2):
                    cols = slice(core * HEAD_DIM, core * HEAD_DIM + HEAD_DIM)
                    for b in range(4):
                        rows = slice(b * SHARE, b * SHARE + SHARE)
                        to = slice(n * SHARE, n * SHARE + SHARE)
                        o_ref[b // 2, core, b % 2, g * (GROUPS // 2) + pair, to] = both[rows, cols]


def pack(queries, key_proj, value_proj, out_grad, row_plan, segments):
    outside = pl.BlockSpec(memory_space=pltpu.HBM)
    outside_args = (
        row_plan.reshape(1, TOK),
        segments,
        queries,
        out_grad,
        key_proj,
        value_proj,
    )
    return pl.pallas_call(
        pack_kernel,
        in_specs=[outside] * 6,
        out_specs=pl.BlockSpec(memory_space=pltpu.VMEM),
        out_shape=jax.ShapeDtypeStruct((2, 2, 2, 16, IN_ROWS, HEAD_DIM), jnp.bfloat16),
        scratch_shapes=[
            pltpu.VMEM((1, TOK), jnp.int32),
            pltpu.VMEM((1, TOK), jnp.int32),
            pltpu.VMEM(queries.shape, queries.dtype),
            pltpu.VMEM(out_grad.shape, out_grad.dtype),
            pltpu.VMEM(key_proj.shape, key_proj.dtype),
            pltpu.VMEM(value_proj.shape, value_proj.dtype),
            pltpu.SemaphoreType.DMA((4 + 2 * KV_HEADS,)),
        ],
        compiler_params=pltpu.CompilerParams(vmem_limit_bytes=16 << 20),
        name="pack",
    )(*(pltpu.with_memory_space_constraint(x, pltpu.HBM) for x in outside_args))


def unpack_kernel(plan_ref, y_ref, att_ref, qg_ref, kg_ref, vg_ref):
    put = plan_matrix(plan_ref).astype(jnp.bfloat16)

    base = pl.program_id(0) * (GROUPS // 2)

    def slots(core, pair, first):
        parts = [
            y_ref[b // 2, core, b % 2, base + pair, slice(first, first + SHARE)] for b in range(4)
        ]
        return jnp.concatenate(parts, axis=0)

    k_sum = jnp.zeros((TOK, HEAD_DIM), jnp.float32)
    v_sum = jnp.zeros((TOK, HEAD_DIM), jnp.float32)
    for pair in range(GROUPS // 2):
        for core in range(2):
            at = slice((pair * 2 + core) * HEAD_DIM, (pair * 2 + core + 1) * HEAD_DIM)
            att_ref[:, at] = dot(put, slots(core, pair, 0)).astype(jnp.bfloat16)
            qg_ref[:, at] = dot(put, slots(core, pair, 32)).astype(jnp.bfloat16)
        k_sum = k_sum + slots(0, pair, 64).astype(jnp.float32)
        v_sum = v_sum + slots(1, pair, 64).astype(jnp.float32)
    kg_ref[...] = dot(put, k_sum.astype(jnp.bfloat16)).astype(jnp.bfloat16)
    vg_ref[...] = dot(put, v_sum.astype(jnp.bfloat16)).astype(jnp.bfloat16)


def unpack(back, row_plan):
    wide = GROUPS * HEAD_DIM
    return pl.pallas_call(
        unpack_kernel,
        grid=(KV_HEADS,),
        in_specs=[
            pl.BlockSpec((1, TOK), lambda g: (0, 0)),
            pl.BlockSpec(memory_space=pltpu.VMEM),
        ],
        out_specs=[
            pl.BlockSpec((TOK, wide), lambda g: (0, g)),
            pl.BlockSpec((TOK, wide), lambda g: (0, g)),
            pl.BlockSpec((TOK, HEAD_DIM), lambda g: (0, g)),
            pl.BlockSpec((TOK, HEAD_DIM), lambda g: (0, g)),
        ],
        out_shape=[
            jax.ShapeDtypeStruct((TOK, HEADS * HEAD_DIM), jnp.bfloat16),
            jax.ShapeDtypeStruct((TOK, HEADS * HEAD_DIM), jnp.bfloat16),
            jax.ShapeDtypeStruct((TOK, KV_HEADS * HEAD_DIM), jnp.bfloat16),
            jax.ShapeDtypeStruct((TOK, KV_HEADS * HEAD_DIM), jnp.bfloat16),
        ],
        compiler_params=pltpu.CompilerParams(vmem_limit_bytes=16 << 20),
        name="unpack",
    )(row_plan.reshape(1, TOK), back)


def attention_kernel(
    z_ref,
    other_ref,
    o_ref,
    keep_ref,
    give_ref,
    q_s,
    qa_s,
    d_s,
    k_s,
    ka_s,
    v_s,
    dt_s,
    kt_s,
    vt_s,
    p_even,
    p_odd,
    tops_even,
    tops_odd,
    rows_even,
    rows_odd,
    dk_s,
    dv_s,
    ot_s,
    qg_s,
    top_s,
    sum_s,
):
    scaling = HEAD_DIM ** (-0.5)
    to_exp2 = scaling * LOG2E
    tall = (TK // 8, 8, TQ)
    core = lax.axis_index("dp") % 2
    group = (lax.axis_index("dp") // 2) * 2 + lax.axis_index("ctx") // 16

    ids = z_ref[group, :, 96:104].astype(jnp.float32)
    cuts = [
        (jnp.sum((ids < float(doc)).astype(jnp.float32)) * 0.125).astype(jnp.int32)
        for doc in range(1, DOCS)
    ]

    lane = lax.broadcasted_iota(jnp.int32, (1, HEAD_DIM), 1)
    ends = jnp.zeros((1, HEAD_DIM), jnp.int32)
    for n, cut in enumerate(cuts):
        ends = jnp.where(lane == n, cut, ends)
    used = lane < DOCS - 1

    def lay_out(c, carry):
        at = pl.ds(pl.multiple_of(c * TOK, TOK), TOK)
        mine = z_ref[:, c, 64:96, :].reshape(TOK, HEAD_DIM)
        theirs = other_ref[:, c].reshape(TOK, HEAD_DIM)
        key_tile = jnp.where(core == 0, mine, theirs)
        value_tile = jnp.where(core == 0, theirs, mine)
        d_tile = z_ref[:, c, SHARE : 2 * SHARE, :].reshape(TOK, HEAD_DIM)
        q_s[at, :] = z_ref[:, c, 0:SHARE, :].reshape(TOK, HEAD_DIM)
        k_s[at, :] = key_tile
        v_s[at, :] = value_tile
        d_s[at, :] = d_tile
        kt_s[c] = key_tile.T
        vt_s[c] = value_tile.T
        dt_s[c] = d_tile.T
        spot = c * TOK + lax.broadcasted_iota(jnp.int32, (TOK, HEAD_DIM), 0)
        early = spot < ends
        qa_s[at, :] = jnp.where(used & ~early, NEG, 0.0).astype(jnp.bfloat16)
        ka_s[at, :] = jnp.where(used & early, 1.0, 0.0).astype(jnp.bfloat16)
        dk_s[at, :] = jnp.zeros((TOK, HEAD_DIM), jnp.float32)
        dv_s[at, :] = jnp.zeros((TOK, HEAD_DIM), jnp.float32)
        return carry

    lax.fori_loop(0, SEQ // TOK, lay_out, 0, unroll=4)

    def doc_start(position):
        start = jnp.zeros_like(position)
        for cut in cuts:
            start = jnp.maximum(start, jnp.where(position >= cut, cut, 0))
        return start

    def chunks(i):
        first_row = i * TQ
        return doc_start(first_row) // TK, (first_row + TQ - 1) // TK + 1

    def key_at(j):
        return pl.ds(pl.multiple_of(j * TK, TK), TK)

    def query_at(i):
        return pl.ds(pl.multiple_of(i * TQ, TQ), TQ)

    def side_by_side(cols_s, first, count):
        return jnp.concatenate([cols_s[first + n] for n in range(count)], axis=1)

    def clear_forward():
        top_s[...] = jnp.full((8, TQ), NEG, jnp.float32)
        sum_s[...] = jnp.zeros((8, TQ), jnp.float32)
        ot_s[...] = jnp.zeros((HEAD_DIM, TQ), jnp.float32)

    def scores_of(i, j, p_s):
        k_at, q_at = key_at(j), query_at(i)
        keys = jnp.concatenate([k_s[k_at, :], ka_s[k_at, :]], axis=1)
        scores = dot_nt(keys, jnp.concatenate([q_s[q_at, :], qa_s[q_at, :]], axis=1))
        rows = i * TQ - j * TK + lax.broadcasted_iota(jnp.int32, (1, TQ), 1)
        keys = lax.broadcasted_iota(jnp.int32, (TK, TQ), 0)
        return jnp.where(keys <= rows, scores, NEG).reshape(tall)

    def soften(scores, j, p_s, tops_s):
        before = top_s[...]
        here = jnp.max(jnp.max(scores, axis=0), axis=0, keepdims=True)
        top = jnp.maximum(before, jnp.broadcast_to(here, (8, TQ)))
        part = jnp.exp2((scores - top) * to_exp2)
        fade = jnp.exp2((before - top) * to_exp2)
        sum_s[...] = sum_s[...] * fade + jnp.sum(part, axis=0)
        top_s[...] = top
        tops_s[j] = top
        part = part.reshape(TK, TQ)
        p_s[key_at(j), :] = part
        return part.astype(jnp.bfloat16), fade

    def add_out(j, part, fade):
        faded = (ot_s[...].reshape(HEAD_DIM // 8, 8, TQ) * fade).reshape(HEAD_DIM, TQ)
        ot_s[...] = faded + dot(side_by_side(vt_s, j * (TK // TOK), TK // TOK), part)

    def forward_step(i, j, p_s, tops_s):
        part, fade = soften(scores_of(i, j, p_s), j, p_s, tops_s)
        add_out(j, part, fade)

    def both_steps(i, j, p_s, tops_s, i_now, j_now, p_now, tops_now, rows_now):
        scores = scores_of(i, j, p_s)
        k_at, q_at = key_at(j_now), query_at(i_now)
        dprobs = dot_nt(v_s[k_at, :], d_s[q_at, :]).reshape(tall)
        share = jnp.exp2((tops_now[j_now] - rows_now[0]) * to_exp2) * rows_now[1]
        held = p_now[k_at, :].reshape(tall)
        weights = (held * share).reshape(TK, TQ).astype(jnp.bfloat16)
        dv_s[k_at, :] += dot(weights, d_s[q_at, :])
        part, fade = soften(scores, j, p_s, tops_s)
        dscore = (held * (share * scaling)) * (dprobs - rows_now[2])
        dscore = dscore.reshape(TK, TQ).astype(jnp.bfloat16)
        dk_s[k_at, :] += dot(dscore, q_s[q_at, :])
        qg_s[...] += dot(side_by_side(kt_s, j_now * (TK // TOK), TK // TOK), dscore)
        add_out(j, part, fade)

    def forward_end(i, rows_s):
        share = 1.0 / jnp.sum(sum_s[...], axis=0, keepdims=True)
        out_t = ot_s[...] * share
        dt = side_by_side(dt_s, i * (TQ // TOK), TQ // TOK)
        row_dot = jnp.sum(dt.astype(jnp.float32) * out_t, axis=0, keepdims=True)
        rows_s[0] = top_s[...]
        rows_s[1] = jnp.broadcast_to(share, (8, TQ))
        rows_s[2] = jnp.broadcast_to(row_dot, (8, TQ))
        out_rows = out_t.astype(jnp.bfloat16).T
        for n in range(TQ // TOK):
            tile = out_rows[n * TOK : n * TOK + TOK].reshape(4, SHARE, HEAD_DIM)
            o_ref[:, i * (TQ // TOK) + n, 0:32] = tile
        clear_forward()

    def gradient_step(i, j, p_s, tops_s, rows_s):
        k_at, q_at = key_at(j), query_at(i)
        share = jnp.exp2((tops_s[j] - rows_s[0]) * to_exp2) * rows_s[1]
        dprobs = dot_nt(v_s[k_at, :], d_s[q_at, :]).reshape(tall)
        part = p_s[k_at, :].reshape(tall)
        weights = (part * share).reshape(TK, TQ).astype(jnp.bfloat16)
        dv_s[k_at, :] += dot(weights, d_s[q_at, :])
        dscore = (part * (share * scaling)) * (dprobs - rows_s[2])
        dscore = dscore.reshape(TK, TQ).astype(jnp.bfloat16)
        dk_s[k_at, :] += dot(dscore, q_s[q_at, :])
        qg_s[...] += dot(side_by_side(kt_s, j * (TK // TOK), TK // TOK), dscore)

    def gradient_end(i):
        grad_rows = qg_s[...].astype(jnp.bfloat16).T
        for n in range(TQ // TOK):
            tile = grad_rows[n * TOK : n * TOK + TOK].reshape(4, SHARE, HEAD_DIM)
            o_ref[:, i * (TQ // TOK) + n, 32:64] = tile
        qg_s[...] = jnp.zeros((HEAD_DIM, TQ), jnp.float32)

    even = (p_even, tops_even, rows_even)
    odd = (p_odd, tops_odd, rows_odd)

    def stage(i_next, ahead, i_now, behind):
        now_lo, now_hi = chunks(i_now)
        next_lo, next_hi = chunks(jnp.minimum(i_next, SEQ // TQ - 1))
        next_n = jnp.where(i_next < SEQ // TQ, next_hi - next_lo, 0)
        now_n = now_hi - now_lo
        both = jnp.minimum(next_n, now_n)

        def together(t, carry):
            both_steps(i_next, next_lo + t, *ahead[:2], i_now, now_lo + t, *behind)
            return carry

        def ahead_only(t, carry):
            forward_step(i_next, next_lo + t, *ahead[:2])
            return carry

        def behind_only(t, carry):
            gradient_step(i_now, now_lo + t, *behind)
            return carry

        lax.fori_loop(0, both, together, 0)
        lax.fori_loop(both, next_n, ahead_only, 0)
        lax.fori_loop(both, now_n, behind_only, 0)

        @pl.when(i_next < SEQ // TQ)
        def _():
            forward_end(i_next, ahead[2])

        gradient_end(i_now)

    clear_forward()
    qg_s[...] = jnp.zeros((HEAD_DIM, TQ), jnp.float32)
    forward_step(0, 0, *even[:2])
    forward_end(0, rows_even)

    def two_stages(m, carry):
        stage(2 * m + 1, odd, 2 * m, even)
        stage(2 * m + 2, even, 2 * m + 1, odd)
        return carry

    lax.fori_loop(0, SEQ // TQ // 2, two_stages, 0)

    def give_back(c, carry):
        at = pl.ds(pl.multiple_of(c * TOK, TOK), TOK)
        k_part = dk_s[at, :].astype(jnp.bfloat16)
        v_part = dv_s[at, :].astype(jnp.bfloat16)
        keep_ref[:, c] = jnp.where(core == 0, k_part, v_part).reshape(4, SHARE, HEAD_DIM)
        give_ref[:, c] = jnp.where(core == 0, v_part, k_part).reshape(4, SHARE, HEAD_DIM)
        return carry

    lax.fori_loop(0, SEQ // TOK, give_back, 0, unroll=4)


def attention(z, other):
    tall = pltpu.VMEM((SEQ, HEAD_DIM), jnp.bfloat16)
    flat = pltpu.VMEM((SEQ // TOK, TOK, HEAD_DIM), jnp.bfloat16)
    whole = pl.BlockSpec(memory_space=pltpu.VMEM)
    part = jax.ShapeDtypeStruct((4, 32, SHARE, HEAD_DIM), jnp.bfloat16)
    return pl.pallas_call(
        attention_kernel,
        in_specs=[whole, whole],
        out_specs=[whole, whole, whole],
        out_shape=[jax.ShapeDtypeStruct((4, 32, 2 * SHARE, HEAD_DIM), jnp.bfloat16), part, part],
        scratch_shapes=[tall] * 6
        + [flat] * 3
        + [pltpu.VMEM((SEQ, TQ), jnp.float32)] * 2
        + [pltpu.VMEM((SEQ // TK, 8, TQ), jnp.float32)] * 2
        + [pltpu.VMEM((3, 8, TQ), jnp.float32)] * 2
        + [pltpu.VMEM((SEQ, HEAD_DIM), jnp.float32)] * 2
        + [pltpu.VMEM((HEAD_DIM, TQ), jnp.float32)] * 2
        + [pltpu.VMEM((8, TQ), jnp.float32)] * 2,
        compiler_params=pltpu.CompilerParams(vmem_limit_bytes=36 << 20),
        name="attention",
    )(z, other)


def join_kernel(rows_ref, keep_ref, got_ref, out_ref):
    def step(c, carry):
        out_ref[:, c, 0:64] = rows_ref[:, c]
        both = keep_ref[:, c].astype(jnp.float32) + got_ref[:, c].astype(jnp.float32)
        out_ref[:, c, 64:96] = both.astype(jnp.bfloat16)
        return carry

    lax.fori_loop(0, 32, step, 0, unroll=4)


def join(rows, keep, got):
    whole = pl.BlockSpec(memory_space=pltpu.VMEM)
    return pl.pallas_call(
        join_kernel,
        in_specs=[whole] * 3,
        out_specs=whole,
        out_shape=jax.ShapeDtypeStruct((4, 32, OUT_ROWS, HEAD_DIM), jnp.bfloat16),
        compiler_params=pltpu.CompilerParams(vmem_limit_bytes=16 << 20),
        name="join",
    )(rows, keep, got)


def to_other_core(x):
    return lax.ppermute(x, "dp", [(0, 1), (1, 0), (2, 3), (3, 2)])


def on_device(queries, key_proj, value_proj, out_grad, row_plan, segments):
    sent = pack(queries, key_proj, value_proj, out_grad, row_plan, segments)
    here = lax.all_to_all(
        sent.reshape(TOK, IN_ROWS, HEAD_DIM), ("dp", "ctx"), split_axis=0, concat_axis=0, tiled=True
    ).reshape(4, 32, IN_ROWS, HEAD_DIM)
    other = to_other_core(here[:, :, 64:96, :])
    rows, keep, give = attention(here, other)
    done = join(rows, keep, to_other_core(give))
    back = lax.all_to_all(
        done.reshape(TOK, OUT_ROWS, HEAD_DIM), ("dp", "ctx"), split_axis=0, concat_axis=0, tiled=True
    )
    return tuple(unpack(back.reshape(2, 2, 2, 16, OUT_ROWS, HEAD_DIM), row_plan))


def solution(mesh):
    rows = P(("dp", "ctx"), None)
    return jax.shard_map(
        on_device,
        mesh=mesh,
        in_specs=(rows, rows, rows, rows, P(("dp", "ctx")), P("dp", "ctx")),
        out_specs=(rows, rows, rows, rows),
        check_vma=False,
    )
```

```python
import functools

import jax
import jax.numpy as jnp
from jax import lax
from jax.experimental import pallas as pl
from jax.experimental.pallas import tpu as pltpu
from jax.sharding import PartitionSpec as P

HEADS = 32
KV_HEADS = 4
HEAD_DIM = 128
GROUPS = HEADS // KV_HEADS
DOCS = 6
NEG = -1e30
LOG2E = 1.4426950408889634
SHARE = 32
TOK = 128
SEQ = 4096
TQ = 256
TK = 512
PAD = TK - TQ
TILES = SEQ // TQ

IN_ROWS = 3 * SHARE + 8
OUT_ROWS = 3 * SHARE


def dot(a, b):
    return jnp.dot(a, b, preferred_element_type=jnp.float32)


def dot_nt(a, b):
    return lax.dot_general(a, b, (((1,), (1,)), ((), ())), preferred_element_type=jnp.float32)


def plan_matrix(plan_ref):
    rows = lax.broadcasted_iota(jnp.int32, (TOK, TOK), 0)
    return jnp.where(rows == plan_ref[...], 1.0, 0.0).astype(jnp.float32)


def pack_kernel(
    plan_hbm,
    seg_hbm,
    q_hbm,
    d_hbm,
    k_hbm,
    v_hbm,
    o_ref,
    plan_ref,
    seg_ref,
    q_ref,
    d_ref,
    k_ref,
    v_ref,
    sems,
):
    small = [
        pltpu.make_async_copy(plan_hbm, plan_ref, sems.at[0]),
        pltpu.make_async_copy(k_hbm, k_ref, sems.at[1]),
        pltpu.make_async_copy(v_hbm, v_ref, sems.at[2]),
        pltpu.make_async_copy(seg_hbm, seg_ref, sems.at[3]),
    ]
    for copy in small:
        copy.start()
    large = []
    for g in range(KV_HEADS):
        at = pl.ds(g * GROUPS * HEAD_DIM, GROUPS * HEAD_DIM)
        large.append(
            (
                pltpu.make_async_copy(q_hbm.at[:, at], q_ref.at[:, at], sems.at[4 + 2 * g]),
                pltpu.make_async_copy(d_hbm.at[:, at], d_ref.at[:, at], sems.at[5 + 2 * g]),
            )
        )
        for copy in large[g]:
            copy.start()
    for copy in small:
        copy.wait()
    pick = plan_matrix(plan_ref).T.astype(jnp.bfloat16)
    seg_rows = jnp.broadcast_to(seg_ref[...].astype(jnp.float32), (8, TOK)).astype(jnp.bfloat16)
    for g in range(KV_HEADS):
        cols = slice(g * HEAD_DIM, g * HEAD_DIM + HEAD_DIM)
        k_rows = dot(pick, k_ref[:, cols]).astype(jnp.bfloat16)
        v_rows = dot(pick, v_ref[:, cols]).astype(jnp.bfloat16)
        for pair in range(GROUPS // 2):
            for core in range(2):
                for b in range(4):
                    rows = slice(b * SHARE, b * SHARE + SHARE)
                    o_ref[b // 2, core, b % 2, g * (GROUPS // 2) + pair, 64:96] = (k_rows, v_rows)[
                        core
                    ][rows]
                    o_ref[b // 2, core, b % 2, g * (GROUPS // 2) + pair, 96:104] = seg_rows
        for n, (copy, ref) in enumerate(zip(large[g], (q_ref, d_ref))):
            copy.wait()
            for pair in range(GROUPS // 2):
                first = (g * (GROUPS // 2) + pair) * 2 * HEAD_DIM
                both = dot(pick, ref[:, first : first + 2 * HEAD_DIM]).astype(jnp.bfloat16)
                for core in range(2):
                    cols = slice(core * HEAD_DIM, core * HEAD_DIM + HEAD_DIM)
                    for b in range(4):
                        rows = slice(b * SHARE, b * SHARE + SHARE)
                        to = slice(n * SHARE, n * SHARE + SHARE)
                        o_ref[b // 2, core, b % 2, g * (GROUPS // 2) + pair, to] = both[rows, cols]


def pack(queries, key_proj, value_proj, out_grad, row_plan, segments):
    outside = pl.BlockSpec(memory_space=pltpu.HBM)
    outside_args = (
        row_plan.reshape(1, TOK),
        segments,
        queries,
        out_grad,
        key_proj,
        value_proj,
    )
    return pl.pallas_call(
        pack_kernel,
        in_specs=[outside] * 6,
        out_specs=pl.BlockSpec(memory_space=pltpu.VMEM),
        out_shape=jax.ShapeDtypeStruct((2, 2, 2, 16, IN_ROWS, HEAD_DIM), jnp.bfloat16),
        scratch_shapes=[
            pltpu.VMEM((1, TOK), jnp.int32),
            pltpu.VMEM((1, TOK), jnp.int32),
            pltpu.VMEM(queries.shape, queries.dtype),
            pltpu.VMEM(out_grad.shape, out_grad.dtype),
            pltpu.VMEM(key_proj.shape, key_proj.dtype),
            pltpu.VMEM(value_proj.shape, value_proj.dtype),
            pltpu.SemaphoreType.DMA((4 + 2 * KV_HEADS,)),
        ],
        compiler_params=pltpu.CompilerParams(vmem_limit_bytes=16 << 20),
        name="pack",
    )(*(pltpu.with_memory_space_constraint(x, pltpu.HBM) for x in outside_args))


def unpack_kernel(plan_ref, y_ref, att_ref, qg_ref, kg_ref, vg_ref):
    put = plan_matrix(plan_ref).astype(jnp.bfloat16)

    base = pl.program_id(0) * (GROUPS // 2)

    def slots(core, pair, first):
        parts = [
            y_ref[b // 2, core, b % 2, base + pair, slice(first, first + SHARE)] for b in range(4)
        ]
        return jnp.concatenate(parts, axis=0)

    k_sum = jnp.zeros((TOK, HEAD_DIM), jnp.float32)
    v_sum = jnp.zeros((TOK, HEAD_DIM), jnp.float32)
    for pair in range(GROUPS // 2):
        for core in range(2):
            at = slice((pair * 2 + core) * HEAD_DIM, (pair * 2 + core + 1) * HEAD_DIM)
            att_ref[:, at] = dot(put, slots(core, pair, 0)).astype(jnp.bfloat16)
            qg_ref[:, at] = dot(put, slots(core, pair, 32)).astype(jnp.bfloat16)
        k_sum = k_sum + slots(0, pair, 64).astype(jnp.float32)
        v_sum = v_sum + slots(1, pair, 64).astype(jnp.float32)
    kg_ref[...] = dot(put, k_sum.astype(jnp.bfloat16)).astype(jnp.bfloat16)
    vg_ref[...] = dot(put, v_sum.astype(jnp.bfloat16)).astype(jnp.bfloat16)


def unpack(back, row_plan):
    wide = GROUPS * HEAD_DIM
    return pl.pallas_call(
        unpack_kernel,
        grid=(KV_HEADS,),
        in_specs=[
            pl.BlockSpec((1, TOK), lambda g: (0, 0)),
            pl.BlockSpec(memory_space=pltpu.VMEM),
        ],
        out_specs=[
            pl.BlockSpec((TOK, wide), lambda g: (0, g)),
            pl.BlockSpec((TOK, wide), lambda g: (0, g)),
            pl.BlockSpec((TOK, HEAD_DIM), lambda g: (0, g)),
            pl.BlockSpec((TOK, HEAD_DIM), lambda g: (0, g)),
        ],
        out_shape=[
            jax.ShapeDtypeStruct((TOK, HEADS * HEAD_DIM), jnp.bfloat16),
            jax.ShapeDtypeStruct((TOK, HEADS * HEAD_DIM), jnp.bfloat16),
            jax.ShapeDtypeStruct((TOK, KV_HEADS * HEAD_DIM), jnp.bfloat16),
            jax.ShapeDtypeStruct((TOK, KV_HEADS * HEAD_DIM), jnp.bfloat16),
        ],
        compiler_params=pltpu.CompilerParams(vmem_limit_bytes=16 << 20),
        name="unpack",
    )(row_plan.reshape(1, TOK), back)


def attention_kernel(
    z_ref,
    other_ref,
    o_ref,
    keep_ref,
    give_ref,
    q_s,
    qa_s,
    d_s,
    k_s,
    ka_s,
    v_s,
    dt_s,
    kt_s,
    vt_s,
    p_even,
    p_odd,
    tops_even,
    tops_odd,
    rows_even,
    rows_odd,
    dk_s,
    dv_s,
    ot_s,
    qg_s,
    top_s,
    sum_s,
):
    scaling = HEAD_DIM ** (-0.5)
    to_exp2 = scaling * LOG2E
    tall = (TK // 8, 8, TQ)
    core = lax.axis_index("dp") % 2
    group = (lax.axis_index("dp") // 2) * 2 + lax.axis_index("ctx") // 16

    ids = z_ref[group, :, 96:104].astype(jnp.float32)
    cuts = [
        (jnp.sum((ids < float(doc)).astype(jnp.float32)) * 0.125).astype(jnp.int32)
        for doc in range(1, DOCS)
    ]

    lane = lax.broadcasted_iota(jnp.int32, (1, HEAD_DIM), 1)
    ends = jnp.zeros((1, HEAD_DIM), jnp.int32)
    for n, cut in enumerate(cuts):
        ends = jnp.where(lane == n, cut, ends)
    used = lane < DOCS - 1

    def lay_out(c, carry):
        at = pl.ds(pl.multiple_of(c * TOK, TOK), TOK)
        key_at = pl.ds(pl.multiple_of(c * TOK + PAD, TOK), TOK)
        mine = z_ref[:, c, 64:96, :].reshape(TOK, HEAD_DIM)
        theirs = other_ref[:, c].reshape(TOK, HEAD_DIM)
        key_tile = jnp.where(core == 0, mine, theirs)
        value_tile = jnp.where(core == 0, theirs, mine)
        d_tile = z_ref[:, c, SHARE : 2 * SHARE, :].reshape(TOK, HEAD_DIM)
        q_s[at, :] = z_ref[:, c, 0:SHARE, :].reshape(TOK, HEAD_DIM)
        k_s[key_at, :] = key_tile
        v_s[key_at, :] = value_tile
        d_s[at, :] = d_tile
        kt_s[c + PAD // TOK] = key_tile.T
        vt_s[c + PAD // TOK] = value_tile.T
        dt_s[c] = d_tile.T
        spot = c * TOK + lax.broadcasted_iota(jnp.int32, (TOK, HEAD_DIM), 0)
        early = spot < ends
        qa_s[at, :] = jnp.where((used & ~early) | (lane == DOCS), NEG, 0.0).astype(jnp.bfloat16)
        ka_s[key_at, :] = jnp.where(used & early, 1.0, 0.0).astype(jnp.bfloat16)
        dk_s[key_at, :] = jnp.zeros((TOK, HEAD_DIM), jnp.float32)
        dv_s[key_at, :] = jnp.zeros((TOK, HEAD_DIM), jnp.float32)
        return carry

    lax.fori_loop(0, SEQ // TOK, lay_out, 0, unroll=4)
    for pad_s in (k_s, v_s, dk_s, dv_s):
        pad_s[:PAD, :] = jnp.zeros((PAD, HEAD_DIM), pad_s.dtype)
    for n in range(PAD // TOK):
        kt_s[n] = jnp.zeros((HEAD_DIM, TOK), jnp.bfloat16)
        vt_s[n] = jnp.zeros((HEAD_DIM, TOK), jnp.bfloat16)
    hidden = jnp.where(jnp.broadcast_to(lane, (PAD, HEAD_DIM)) == DOCS, 1.0, 0.0)
    ka_s[:PAD, :] = hidden.astype(jnp.bfloat16)

    def doc_start(position):
        start = jnp.zeros_like(position)
        for cut in cuts:
            start = jnp.maximum(start, jnp.where(position >= cut, cut, 0))
        return start

    def chunks(i):
        return ((i + 1) * TQ - doc_start(i * TQ) + TK - 1) // TK

    def key_at(i, t):
        return pl.ds(pl.multiple_of(i * TQ - t * TK, TQ), TK)

    def key_blocks(cols_s, i, t):
        return side_by_side(cols_s, (i * TQ - t * TK) // TOK, TK // TOK)

    def query_at(i):
        return pl.ds(pl.multiple_of(i * TQ, TQ), TQ)

    def side_by_side(cols_s, first, count):
        return jnp.concatenate([cols_s[first + n] for n in range(count)], axis=1)

    def clear_forward():
        top_s[...] = jnp.full((8, TQ), NEG, jnp.float32)
        sum_s[...] = jnp.zeros((8, TQ), jnp.float32)
        ot_s[...] = jnp.zeros((HEAD_DIM, TQ), jnp.float32)

    def scores_of(i, t, last):
        k_at, q_at = key_at(i, t), query_at(i)
        keys = jnp.concatenate([k_s[k_at, :], ka_s[k_at, :]], axis=1)
        scores = dot_nt(keys, jnp.concatenate([q_s[q_at, :], qa_s[q_at, :]], axis=1))
        if last:
            ahead = lax.broadcasted_iota(jnp.int32, (TQ, TQ), 0)
            reach = lax.broadcasted_iota(jnp.int32, (TQ, TQ), 1)
            own = jnp.where(ahead <= reach, scores[PAD:], NEG)
            scores = jnp.concatenate([scores[:PAD], own], axis=0)
        return scores.reshape(tall)

    def soften(scores, i, t, p_s, tops_s):
        before = top_s[...]
        here = jnp.max(jnp.max(scores, axis=0), axis=0, keepdims=True)
        top = jnp.maximum(before, jnp.broadcast_to(here, (8, TQ)))
        part = jnp.exp2((scores - top) * to_exp2)
        fade = jnp.exp2((before - top) * to_exp2)
        sum_s[...] = sum_s[...] * fade + jnp.sum(part, axis=0)
        top_s[...] = top
        tops_s[t] = top
        part = part.reshape(TK, TQ)
        p_s[key_at(i, t), :] = part
        return part.astype(jnp.bfloat16), fade

    def add_out(i, t, part, fade):
        faded = (ot_s[...].reshape(HEAD_DIM // 8, 8, TQ) * fade).reshape(HEAD_DIM, TQ)
        ot_s[...] = faded + dot(key_blocks(vt_s, i, t), part)

    def forward_step(i, t, last, p_s, tops_s):
        part, fade = soften(scores_of(i, t, last), i, t, p_s, tops_s)
        add_out(i, t, part, fade)

    def both_steps(i, t, last, p_s, tops_s, i_now, p_now, tops_now, rows_now):
        scores = scores_of(i, t, last)
        k_at, q_at = key_at(i_now, t), query_at(i_now)
        dprobs = dot_nt(v_s[k_at, :], d_s[q_at, :]).reshape(tall)
        share = jnp.exp2((tops_now[t] - rows_now[0]) * to_exp2) * rows_now[1]
        held = p_now[k_at, :].reshape(tall)
        weights = (held * share).reshape(TK, TQ).astype(jnp.bfloat16)
        dv_s[k_at, :] += dot(weights, d_s[q_at, :])
        part, fade = soften(scores, i, t, p_s, tops_s)
        dscore = (held * (share * scaling)) * (dprobs - rows_now[2])
        dscore = dscore.reshape(TK, TQ).astype(jnp.bfloat16)
        dk_s[k_at, :] += dot(dscore, q_s[q_at, :])
        qg_s[...] += dot(key_blocks(kt_s, i_now, t), dscore)
        add_out(i, t, part, fade)

    def forward_end(i, rows_s):
        share = 1.0 / jnp.sum(sum_s[...], axis=0, keepdims=True)
        out_t = ot_s[...] * share
        dt = side_by_side(dt_s, i * (TQ // TOK), TQ // TOK)
        row_dot = jnp.sum(dt.astype(jnp.float32) * out_t, axis=0, keepdims=True)
        rows_s[0] = top_s[...]
        rows_s[1] = jnp.broadcast_to(share, (8, TQ))
        rows_s[2] = jnp.broadcast_to(row_dot, (8, TQ))
        out_rows = out_t.astype(jnp.bfloat16).T
        for n in range(TQ // TOK):
            tile = out_rows[n * TOK : n * TOK + TOK].reshape(4, SHARE, HEAD_DIM)
            o_ref[:, i * (TQ // TOK) + n, 0:32] = tile
        clear_forward()

    def gradient_step(i, t, p_s, tops_s, rows_s):
        k_at, q_at = key_at(i, t), query_at(i)
        share = jnp.exp2((tops_s[t] - rows_s[0]) * to_exp2) * rows_s[1]
        dprobs = dot_nt(v_s[k_at, :], d_s[q_at, :]).reshape(tall)
        part = p_s[k_at, :].reshape(tall)
        weights = (part * share).reshape(TK, TQ).astype(jnp.bfloat16)
        dv_s[k_at, :] += dot(weights, d_s[q_at, :])
        dscore = (part * (share * scaling)) * (dprobs - rows_s[2])
        dscore = dscore.reshape(TK, TQ).astype(jnp.bfloat16)
        dk_s[k_at, :] += dot(dscore, q_s[q_at, :])
        qg_s[...] += dot(key_blocks(kt_s, i, t), dscore)

    def gradient_end(i):
        grad_rows = qg_s[...].astype(jnp.bfloat16).T
        for n in range(TQ // TOK):
            tile = grad_rows[n * TOK : n * TOK + TOK].reshape(4, SHARE, HEAD_DIM)
            o_ref[:, i * (TQ // TOK) + n, 32:64] = tile
        qg_s[...] = jnp.zeros((HEAD_DIM, TQ), jnp.float32)

    even = (p_even, tops_even, rows_even)
    odd = (p_odd, tops_odd, rows_odd)

    def stage(i_next, ahead, i_now, behind):
        now_n = chunks(i_now)
        next_n = jnp.where(i_next < TILES, chunks(jnp.minimum(i_next, TILES - 1)), 0)
        both = jnp.minimum(next_n, now_n)

        def together(t, carry):
            both_steps(i_next, t, False, *ahead[:2], i_now, *behind)
            return carry

        def ahead_only(t, carry):
            forward_step(i_next, t, False, *ahead[:2])
            return carry

        def behind_only(t, carry):
            gradient_step(i_now, t, *behind)
            return carry

        @pl.when(i_next < TILES)
        def _():
            both_steps(i_next, 0, True, *ahead[:2], i_now, *behind)
            lax.fori_loop(1, both, together, 0)
            lax.fori_loop(both, next_n, ahead_only, 0)
            forward_end(i_next, ahead[2])

        lax.fori_loop(both, now_n, behind_only, 0)
        gradient_end(i_now)

    clear_forward()
    qg_s[...] = jnp.zeros((HEAD_DIM, TQ), jnp.float32)
    forward_step(0, 0, True, *even[:2])
    forward_end(0, rows_even)

    def two_stages(m, carry):
        stage(2 * m + 1, odd, 2 * m, even)
        stage(2 * m + 2, even, 2 * m + 1, odd)
        return carry

    lax.fori_loop(0, TILES // 2, two_stages, 0)

    def give_back(c, carry):
        at = pl.ds(pl.multiple_of(c * TOK + PAD, TOK), TOK)
        k_part = dk_s[at, :].astype(jnp.bfloat16)
        v_part = dv_s[at, :].astype(jnp.bfloat16)
        keep_ref[:, c] = jnp.where(core == 0, k_part, v_part).reshape(4, SHARE, HEAD_DIM)
        give_ref[:, c] = jnp.where(core == 0, v_part, k_part).reshape(4, SHARE, HEAD_DIM)
        return carry

    lax.fori_loop(0, SEQ // TOK, give_back, 0, unroll=4)


def attention(z, other):
    tall = pltpu.VMEM((SEQ, HEAD_DIM), jnp.bfloat16)
    keys = pltpu.VMEM((SEQ + PAD, HEAD_DIM), jnp.bfloat16)
    flat = pltpu.VMEM((SEQ // TOK, TOK, HEAD_DIM), jnp.bfloat16)
    key_cols = pltpu.VMEM(((SEQ + PAD) // TOK, TOK, HEAD_DIM), jnp.bfloat16)
    whole = pl.BlockSpec(memory_space=pltpu.VMEM)
    part = jax.ShapeDtypeStruct((4, 32, SHARE, HEAD_DIM), jnp.bfloat16)
    return pl.pallas_call(
        attention_kernel,
        in_specs=[whole, whole],
        out_specs=[whole, whole, whole],
        out_shape=[jax.ShapeDtypeStruct((4, 32, 2 * SHARE, HEAD_DIM), jnp.bfloat16), part, part],
        scratch_shapes=[tall, tall, tall, keys, keys, keys, flat, key_cols, key_cols]
        + [pltpu.VMEM((SEQ + PAD, TQ), jnp.float32)] * 2
        + [pltpu.VMEM((SEQ // TK, 8, TQ), jnp.float32)] * 2
        + [pltpu.VMEM((3, 8, TQ), jnp.float32)] * 2
        + [pltpu.VMEM((SEQ + PAD, HEAD_DIM), jnp.float32)] * 2
        + [pltpu.VMEM((HEAD_DIM, TQ), jnp.float32)] * 2
        + [pltpu.VMEM((8, TQ), jnp.float32)] * 2,
        compiler_params=pltpu.CompilerParams(vmem_limit_bytes=36 << 20),
        name="attention",
    )(z, other)


def join_kernel(rows_ref, keep_ref, got_ref, out_ref):
    def step(c, carry):
        out_ref[:, c, 0:64] = rows_ref[:, c]
        both = keep_ref[:, c].astype(jnp.float32) + got_ref[:, c].astype(jnp.float32)
        out_ref[:, c, 64:96] = both.astype(jnp.bfloat16)
        return carry

    lax.fori_loop(0, 32, step, 0, unroll=4)


def join(rows, keep, got):
    whole = pl.BlockSpec(memory_space=pltpu.VMEM)
    return pl.pallas_call(
        join_kernel,
        in_specs=[whole] * 3,
        out_specs=whole,
        out_shape=jax.ShapeDtypeStruct((4, 32, OUT_ROWS, HEAD_DIM), jnp.bfloat16),
        compiler_params=pltpu.CompilerParams(vmem_limit_bytes=16 << 20),
        name="join",
    )(rows, keep, got)


def to_other_core(x):
    return lax.ppermute(x, "dp", [(0, 1), (1, 0), (2, 3), (3, 2)])


def on_device(queries, key_proj, value_proj, out_grad, row_plan, segments):
    sent = pack(queries, key_proj, value_proj, out_grad, row_plan, segments)
    here = lax.all_to_all(
        sent.reshape(TOK, IN_ROWS, HEAD_DIM), ("dp", "ctx"), split_axis=0, concat_axis=0, tiled=True
    ).reshape(4, 32, IN_ROWS, HEAD_DIM)
    other = to_other_core(here[:, :, 64:96, :])
    rows, keep, give = attention(here, other)
    done = join(rows, keep, to_other_core(give))
    back = lax.all_to_all(
        done.reshape(TOK, OUT_ROWS, HEAD_DIM), ("dp", "ctx"), split_axis=0, concat_axis=0, tiled=True
    )
    return tuple(unpack(back.reshape(2, 2, 2, 16, OUT_ROWS, HEAD_DIM), row_plan))


def solution(mesh):
    rows = P(("dp", "ctx"), None)
    return jax.shard_map(
        on_device,
        mesh=mesh,
        in_specs=(rows, rows, rows, rows, P(("dp", "ctx")), P("dp", "ctx")),
        out_specs=(rows, rows, rows, rows),
        check_vma=False,
    )
```

```python
import functools

import jax
import jax.numpy as jnp
from jax import lax
from jax.experimental import pallas as pl
from jax.experimental.pallas import tpu as pltpu
from jax.sharding import PartitionSpec as P

HEADS = 32
KV_HEADS = 4
HEAD_DIM = 128
GROUPS = HEADS // KV_HEADS
DOCS = 6
NEG = -1e30
LOG2E = 1.4426950408889634
SHARE = 32
TOK = 128
SEQ = 4096
TQ = 256
TK = 512
PAD = TK - TQ
TILES = SEQ // TQ

IN_ROWS = 3 * SHARE + 8
OUT_ROWS = 3 * SHARE


def dot(a, b):
    return jnp.dot(a, b, preferred_element_type=jnp.float32)


def dot_nt(a, b):
    return lax.dot_general(a, b, (((1,), (1,)), ((), ())), preferred_element_type=jnp.float32)


def plan_matrix(plan_ref):
    rows = lax.broadcasted_iota(jnp.int32, (TOK, TOK), 0)
    return jnp.where(rows == plan_ref[...], 1.0, 0.0).astype(jnp.float32)


def pack_kernel(
    plan_hbm,
    seg_hbm,
    q_hbm,
    d_hbm,
    k_hbm,
    v_hbm,
    o_ref,
    plan_ref,
    seg_ref,
    q_ref,
    d_ref,
    k_ref,
    v_ref,
    sems,
):
    small = [
        pltpu.make_async_copy(plan_hbm, plan_ref, sems.at[0]),
        pltpu.make_async_copy(k_hbm, k_ref, sems.at[1]),
        pltpu.make_async_copy(v_hbm, v_ref, sems.at[2]),
        pltpu.make_async_copy(seg_hbm, seg_ref, sems.at[3]),
    ]
    for copy in small:
        copy.start()
    large = []
    for g in range(KV_HEADS):
        at = pl.ds(g * GROUPS * HEAD_DIM, GROUPS * HEAD_DIM)
        large.append(
            (
                pltpu.make_async_copy(q_hbm.at[:, at], q_ref.at[:, at], sems.at[4 + 2 * g]),
                pltpu.make_async_copy(d_hbm.at[:, at], d_ref.at[:, at], sems.at[5 + 2 * g]),
            )
        )
        for copy in large[g]:
            copy.start()
    for copy in small:
        copy.wait()
    pick = plan_matrix(plan_ref).T.astype(jnp.bfloat16)
    seg_rows = jnp.broadcast_to(seg_ref[...].astype(jnp.float32), (8, TOK)).astype(jnp.bfloat16)
    for g in range(KV_HEADS):
        cols = slice(g * HEAD_DIM, g * HEAD_DIM + HEAD_DIM)
        k_rows = dot(pick, k_ref[:, cols]).astype(jnp.bfloat16)
        v_rows = dot(pick, v_ref[:, cols]).astype(jnp.bfloat16)
        for pair in range(GROUPS // 2):
            for core in range(2):
                for b in range(4):
                    rows = slice(b * SHARE, b * SHARE + SHARE)
                    o_ref[b // 2, core, b % 2, g * (GROUPS // 2) + pair, 64:96] = (k_rows, v_rows)[
                        core
                    ][rows]
                    o_ref[b // 2, core, b % 2, g * (GROUPS // 2) + pair, 96:104] = seg_rows
        for n, (copy, ref) in enumerate(zip(large[g], (q_ref, d_ref))):
            copy.wait()
            for pair in range(GROUPS // 2):
                first = (g * (GROUPS // 2) + pair) * 2 * HEAD_DIM
                both = dot(pick, ref[:, first : first + 2 * HEAD_DIM]).astype(jnp.bfloat16)
                for core in range(2):
                    cols = slice(core * HEAD_DIM, core * HEAD_DIM + HEAD_DIM)
                    for b in range(4):
                        rows = slice(b * SHARE, b * SHARE + SHARE)
                        to = slice(n * SHARE, n * SHARE + SHARE)
                        o_ref[b // 2, core, b % 2, g * (GROUPS // 2) + pair, to] = both[rows, cols]


def pack(queries, key_proj, value_proj, out_grad, row_plan, segments):
    outside = pl.BlockSpec(memory_space=pltpu.HBM)
    outside_args = (
        row_plan.reshape(1, TOK),
        segments,
        queries,
        out_grad,
        key_proj,
        value_proj,
    )
    return pl.pallas_call(
        pack_kernel,
        in_specs=[outside] * 6,
        out_specs=pl.BlockSpec(memory_space=pltpu.VMEM),
        out_shape=jax.ShapeDtypeStruct((2, 2, 2, 16, IN_ROWS, HEAD_DIM), jnp.bfloat16),
        scratch_shapes=[
            pltpu.VMEM((1, TOK), jnp.int32),
            pltpu.VMEM((1, TOK), jnp.int32),
            pltpu.VMEM(queries.shape, queries.dtype),
            pltpu.VMEM(out_grad.shape, out_grad.dtype),
            pltpu.VMEM(key_proj.shape, key_proj.dtype),
            pltpu.VMEM(value_proj.shape, value_proj.dtype),
            pltpu.SemaphoreType.DMA((4 + 2 * KV_HEADS,)),
        ],
        compiler_params=pltpu.CompilerParams(vmem_limit_bytes=16 << 20),
        name="pack",
    )(*(pltpu.with_memory_space_constraint(x, pltpu.HBM) for x in outside_args))


def unpack_kernel(plan_ref, y_ref, att_ref, qg_ref, kg_ref, vg_ref):
    put = plan_matrix(plan_ref).astype(jnp.bfloat16)

    base = pl.program_id(0) * (GROUPS // 2)

    def slots(core, pair, first):
        parts = [
            y_ref[b // 2, core, b % 2, base + pair, slice(first, first + SHARE)] for b in range(4)
        ]
        return jnp.concatenate(parts, axis=0)

    k_sum = jnp.zeros((TOK, HEAD_DIM), jnp.float32)
    v_sum = jnp.zeros((TOK, HEAD_DIM), jnp.float32)
    for pair in range(GROUPS // 2):
        for core in range(2):
            at = slice((pair * 2 + core) * HEAD_DIM, (pair * 2 + core + 1) * HEAD_DIM)
            att_ref[:, at] = dot(put, slots(core, pair, 0)).astype(jnp.bfloat16)
            qg_ref[:, at] = dot(put, slots(core, pair, 32)).astype(jnp.bfloat16)
        k_sum = k_sum + slots(0, pair, 64).astype(jnp.float32)
        v_sum = v_sum + slots(1, pair, 64).astype(jnp.float32)
    kg_ref[...] = dot(put, k_sum.astype(jnp.bfloat16)).astype(jnp.bfloat16)
    vg_ref[...] = dot(put, v_sum.astype(jnp.bfloat16)).astype(jnp.bfloat16)


def unpack(back, row_plan):
    wide = GROUPS * HEAD_DIM
    return pl.pallas_call(
        unpack_kernel,
        grid=(KV_HEADS,),
        in_specs=[
            pl.BlockSpec((1, TOK), lambda g: (0, 0)),
            pl.BlockSpec(memory_space=pltpu.VMEM),
        ],
        out_specs=[
            pl.BlockSpec((TOK, wide), lambda g: (0, g)),
            pl.BlockSpec((TOK, wide), lambda g: (0, g)),
            pl.BlockSpec((TOK, HEAD_DIM), lambda g: (0, g)),
            pl.BlockSpec((TOK, HEAD_DIM), lambda g: (0, g)),
        ],
        out_shape=[
            jax.ShapeDtypeStruct((TOK, HEADS * HEAD_DIM), jnp.bfloat16),
            jax.ShapeDtypeStruct((TOK, HEADS * HEAD_DIM), jnp.bfloat16),
            jax.ShapeDtypeStruct((TOK, KV_HEADS * HEAD_DIM), jnp.bfloat16),
            jax.ShapeDtypeStruct((TOK, KV_HEADS * HEAD_DIM), jnp.bfloat16),
        ],
        compiler_params=pltpu.CompilerParams(vmem_limit_bytes=16 << 20),
        name="unpack",
    )(row_plan.reshape(1, TOK), back)


def attention_kernel(
    z_ref,
    other_ref,
    o_ref,
    keep_ref,
    give_ref,
    q_s,
    qa_s,
    d_s,
    k_s,
    ka_s,
    v_s,
    dt_s,
    kt_s,
    vt_s,
    p_even,
    p_odd,
    tops_even,
    tops_odd,
    rows_even,
    rows_odd,
    dk_s,
    dv_s,
    ot_s,
    qg_s,
    top_s,
    sum_s,
):
    scaling = HEAD_DIM ** (-0.5)
    to_exp2 = scaling * LOG2E
    tall = (TK // 8, 8, TQ)
    core = lax.axis_index("dp") % 2
    group = (lax.axis_index("dp") // 2) * 2 + lax.axis_index("ctx") // 16

    ids = z_ref[group, :, 96:104].astype(jnp.float32)
    cuts = [
        (jnp.sum((ids < float(doc)).astype(jnp.float32)) * 0.125).astype(jnp.int32)
        for doc in range(1, DOCS)
    ]

    lane = lax.broadcasted_iota(jnp.int32, (1, HEAD_DIM), 1)
    ends = jnp.zeros((1, HEAD_DIM), jnp.int32)
    for n, cut in enumerate(cuts):
        ends = jnp.where(lane == n, cut, ends)
    used = lane < DOCS - 1

    def lay_out(c, carry):
        at = pl.ds(pl.multiple_of(c * TOK, TOK), TOK)
        key_at = pl.ds(pl.multiple_of(c * TOK + PAD, TOK), TOK)
        mine = z_ref[:, c, 64:96, :].reshape(TOK, HEAD_DIM)
        theirs = other_ref[:, c].reshape(TOK, HEAD_DIM)
        key_tile = jnp.where(core == 0, mine, theirs)
        value_tile = jnp.where(core == 0, theirs, mine)
        d_tile = z_ref[:, c, SHARE : 2 * SHARE, :].reshape(TOK, HEAD_DIM)
        q_s[at, :] = z_ref[:, c, 0:SHARE, :].reshape(TOK, HEAD_DIM)
        k_s[key_at, :] = key_tile
        v_s[key_at, :] = value_tile
        d_s[at, :] = d_tile
        kt_s[c + PAD // TOK] = key_tile.T
        vt_s[c + PAD // TOK] = value_tile.T
        dt_s[c] = d_tile.T
        dk_s[key_at, :] = jnp.zeros((TOK, HEAD_DIM), jnp.float32)
        dv_s[key_at, :] = jnp.zeros((TOK, HEAD_DIM), jnp.float32)
        return carry

    lax.fori_loop(0, SEQ // TOK, lay_out, 0, unroll=4)

    def mark(c, carry):
        at = pl.ds(pl.multiple_of(c * TOK, TOK), TOK)
        key_at = pl.ds(pl.multiple_of(c * TOK + PAD, TOK), TOK)
        spot = c * TOK + lax.broadcasted_iota(jnp.int32, (TOK, HEAD_DIM), 0)
        early = spot < ends
        qa_s[at, :] = jnp.where((used & ~early) | (lane == DOCS), NEG, 0.0).astype(jnp.bfloat16)
        ka_s[key_at, :] = jnp.where(used & early, 1.0, 0.0).astype(jnp.bfloat16)
        return carry

    lax.fori_loop(0, SEQ // TOK, mark, 0, unroll=2)
    for pad_s in (k_s, v_s, dk_s, dv_s):
        pad_s[:PAD, :] = jnp.zeros((PAD, HEAD_DIM), pad_s.dtype)
    for n in range(PAD // TOK):
        kt_s[n] = jnp.zeros((HEAD_DIM, TOK), jnp.bfloat16)
        vt_s[n] = jnp.zeros((HEAD_DIM, TOK), jnp.bfloat16)
    hidden = jnp.where(jnp.broadcast_to(lane, (PAD, HEAD_DIM)) == DOCS, 1.0, 0.0)
    ka_s[:PAD, :] = hidden.astype(jnp.bfloat16)

    def doc_start(position):
        start = jnp.zeros_like(position)
        for cut in cuts:
            start = jnp.maximum(start, jnp.where(position >= cut, cut, 0))
        return start

    def chunks(i):
        return ((i + 1) * TQ - doc_start(i * TQ) + TK - 1) // TK

    def key_at(i, t):
        return pl.ds(pl.multiple_of(i * TQ - t * TK, TQ), TK)

    def key_blocks(cols_s, i, t):
        return side_by_side(cols_s, (i * TQ - t * TK) // TOK, TK // TOK)

    def query_at(i):
        return pl.ds(pl.multiple_of(i * TQ, TQ), TQ)

    def side_by_side(cols_s, first, count):
        return jnp.concatenate([cols_s[first + n] for n in range(count)], axis=1)

    def clear_forward():
        top_s[...] = jnp.full((8, TQ), NEG, jnp.float32)
        sum_s[...] = jnp.zeros((8, TQ), jnp.float32)
        ot_s[...] = jnp.zeros((HEAD_DIM, TQ), jnp.float32)

    def scores_of(i, t, last):
        k_at, q_at = key_at(i, t), query_at(i)
        keys = jnp.concatenate([k_s[k_at, :], ka_s[k_at, :]], axis=1)
        scores = dot_nt(keys, jnp.concatenate([q_s[q_at, :], qa_s[q_at, :]], axis=1))
        if last:
            ahead = lax.broadcasted_iota(jnp.int32, (TQ, TQ), 0)
            reach = lax.broadcasted_iota(jnp.int32, (TQ, TQ), 1)
            own = jnp.where(ahead <= reach, scores[PAD:], NEG)
            scores = jnp.concatenate([scores[:PAD], own], axis=0)
        return scores.reshape(tall)

    def soften(scores, i, t, p_s, tops_s):
        before = top_s[...]
        here = jnp.max(jnp.max(scores, axis=0), axis=0, keepdims=True)
        top = jnp.maximum(before, jnp.broadcast_to(here, (8, TQ)))
        part = jnp.exp2((scores - top) * to_exp2)
        fade = jnp.exp2((before - top) * to_exp2)
        sum_s[...] = sum_s[...] * fade + jnp.sum(part, axis=0)
        top_s[...] = top
        tops_s[t] = top
        part = part.reshape(TK, TQ)
        p_s[key_at(i, t), :] = part
        return part.astype(jnp.bfloat16), fade

    def add_out(i, t, part, fade):
        faded = (ot_s[...].reshape(HEAD_DIM // 8, 8, TQ) * fade).reshape(HEAD_DIM, TQ)
        ot_s[...] = faded + dot(key_blocks(vt_s, i, t), part)

    def forward_step(i, t, last, p_s, tops_s):
        part, fade = soften(scores_of(i, t, last), i, t, p_s, tops_s)
        add_out(i, t, part, fade)

    def both_steps(i, t, last, p_s, tops_s, i_now, p_now, tops_now, rows_now):
        scores = scores_of(i, t, last)
        k_at, q_at = key_at(i_now, t), query_at(i_now)
        dprobs = dot_nt(v_s[k_at, :], d_s[q_at, :]).reshape(tall)
        share = jnp.exp2((tops_now[t] - rows_now[0]) * to_exp2) * rows_now[1]
        held = p_now[k_at, :].reshape(tall)
        weights = (held * share).reshape(TK, TQ).astype(jnp.bfloat16)
        dv_s[k_at, :] += dot(weights, d_s[q_at, :])
        part, fade = soften(scores, i, t, p_s, tops_s)
        dscore = (held * (share * scaling)) * (dprobs - rows_now[2])
        dscore = dscore.reshape(TK, TQ).astype(jnp.bfloat16)
        dk_s[k_at, :] += dot(dscore, q_s[q_at, :])
        qg_s[...] += dot(key_blocks(kt_s, i_now, t), dscore)
        add_out(i, t, part, fade)

    def forward_end(i, rows_s):
        share = 1.0 / jnp.sum(sum_s[...], axis=0, keepdims=True)
        out_t = ot_s[...] * share
        dt = side_by_side(dt_s, i * (TQ // TOK), TQ // TOK)
        row_dot = jnp.sum(dt.astype(jnp.float32) * out_t, axis=0, keepdims=True)
        rows_s[0] = top_s[...]
        rows_s[1] = jnp.broadcast_to(share, (8, TQ))
        rows_s[2] = jnp.broadcast_to(row_dot, (8, TQ))
        out_rows = out_t.astype(jnp.bfloat16).T
        for n in range(TQ // TOK):
            tile = out_rows[n * TOK : n * TOK + TOK].reshape(4, SHARE, HEAD_DIM)
            o_ref[:, i * (TQ // TOK) + n, 0:32] = tile
        clear_forward()

    def gradient_step(i, t, p_s, tops_s, rows_s):
        k_at, q_at = key_at(i, t), query_at(i)
        share = jnp.exp2((tops_s[t] - rows_s[0]) * to_exp2) * rows_s[1]
        dprobs = dot_nt(v_s[k_at, :], d_s[q_at, :]).reshape(tall)
        part = p_s[k_at, :].reshape(tall)
        weights = (part * share).reshape(TK, TQ).astype(jnp.bfloat16)
        dv_s[k_at, :] += dot(weights, d_s[q_at, :])
        dscore = (part * (share * scaling)) * (dprobs - rows_s[2])
        dscore = dscore.reshape(TK, TQ).astype(jnp.bfloat16)
        dk_s[k_at, :] += dot(dscore, q_s[q_at, :])
        qg_s[...] += dot(key_blocks(kt_s, i, t), dscore)

    def gradient_end(i):
        grad_rows = qg_s[...].astype(jnp.bfloat16).T
        for n in range(TQ // TOK):
            tile = grad_rows[n * TOK : n * TOK + TOK].reshape(4, SHARE, HEAD_DIM)
            o_ref[:, i * (TQ // TOK) + n, 32:64] = tile
        qg_s[...] = jnp.zeros((HEAD_DIM, TQ), jnp.float32)

    even = (p_even, tops_even, rows_even)
    odd = (p_odd, tops_odd, rows_odd)

    def stage(i_next, ahead, i_now, behind):
        now_n = chunks(i_now)
        next_n = jnp.where(i_next < TILES, chunks(jnp.minimum(i_next, TILES - 1)), 0)
        both = jnp.minimum(next_n, now_n)

        def together(t, carry):
            both_steps(i_next, t, False, *ahead[:2], i_now, *behind)
            return carry

        def ahead_only(t, carry):
            forward_step(i_next, t, False, *ahead[:2])
            return carry

        def behind_only(t, carry):
            gradient_step(i_now, t, *behind)
            return carry

        @pl.when(i_next < TILES)
        def _():
            both_steps(i_next, 0, True, *ahead[:2], i_now, *behind)
            lax.fori_loop(1, both, together, 0)
            lax.fori_loop(both, next_n, ahead_only, 0)
            forward_end(i_next, ahead[2])

        lax.fori_loop(both, now_n, behind_only, 0)
        gradient_end(i_now)

    clear_forward()
    qg_s[...] = jnp.zeros((HEAD_DIM, TQ), jnp.float32)
    forward_step(0, 0, True, *even[:2])
    forward_end(0, rows_even)

    def two_stages(m, carry):
        stage(2 * m + 1, odd, 2 * m, even)
        stage(2 * m + 2, even, 2 * m + 1, odd)
        return carry

    lax.fori_loop(0, TILES // 2, two_stages, 0)

    def give_back(c, carry):
        at = pl.ds(pl.multiple_of(c * TOK + PAD, TOK), TOK)
        k_part = dk_s[at, :].astype(jnp.bfloat16)
        v_part = dv_s[at, :].astype(jnp.bfloat16)
        keep_ref[:, c] = jnp.where(core == 0, k_part, v_part).reshape(4, SHARE, HEAD_DIM)
        give_ref[:, c] = jnp.where(core == 0, v_part, k_part).reshape(4, SHARE, HEAD_DIM)
        return carry

    lax.fori_loop(0, SEQ // TOK, give_back, 0, unroll=4)


def attention(z, other):
    tall = pltpu.VMEM((SEQ, HEAD_DIM), jnp.bfloat16)
    keys = pltpu.VMEM((SEQ + PAD, HEAD_DIM), jnp.bfloat16)
    flat = pltpu.VMEM((SEQ // TOK, TOK, HEAD_DIM), jnp.bfloat16)
    key_cols = pltpu.VMEM(((SEQ + PAD) // TOK, TOK, HEAD_DIM), jnp.bfloat16)
    whole = pl.BlockSpec(memory_space=pltpu.VMEM)
    part = jax.ShapeDtypeStruct((4, 32, SHARE, HEAD_DIM), jnp.bfloat16)
    return pl.pallas_call(
        attention_kernel,
        in_specs=[whole, whole],
        out_specs=[whole, whole, whole],
        out_shape=[jax.ShapeDtypeStruct((4, 32, 2 * SHARE, HEAD_DIM), jnp.bfloat16), part, part],
        scratch_shapes=[tall, tall, tall, keys, keys, keys, flat, key_cols, key_cols]
        + [pltpu.VMEM((SEQ + PAD, TQ), jnp.float32)] * 2
        + [pltpu.VMEM((SEQ // TK, 8, TQ), jnp.float32)] * 2
        + [pltpu.VMEM((3, 8, TQ), jnp.float32)] * 2
        + [pltpu.VMEM((SEQ + PAD, HEAD_DIM), jnp.float32)] * 2
        + [pltpu.VMEM((HEAD_DIM, TQ), jnp.float32)] * 2
        + [pltpu.VMEM((8, TQ), jnp.float32)] * 2,
        compiler_params=pltpu.CompilerParams(
            vmem_limit_bytes=36 << 20
        ),
        name="attention",
    )(z, other)


def join_kernel(rows_ref, keep_ref, got_ref, out_ref):
    def step(c, carry):
        out_ref[:, c, 0:64] = rows_ref[:, c]
        both = keep_ref[:, c].astype(jnp.float32) + got_ref[:, c].astype(jnp.float32)
        out_ref[:, c, 64:96] = both.astype(jnp.bfloat16)
        return carry

    lax.fori_loop(0, 32, step, 0, unroll=4)


def join(rows, keep, got):
    whole = pl.BlockSpec(memory_space=pltpu.VMEM)
    return pl.pallas_call(
        join_kernel,
        in_specs=[whole] * 3,
        out_specs=whole,
        out_shape=jax.ShapeDtypeStruct((4, 32, OUT_ROWS, HEAD_DIM), jnp.bfloat16),
        compiler_params=pltpu.CompilerParams(vmem_limit_bytes=16 << 20),
        name="join",
    )(rows, keep, got)


def to_other_core(x):
    return lax.ppermute(x, "dp", [(0, 1), (1, 0), (2, 3), (3, 2)])


def on_device(queries, key_proj, value_proj, out_grad, row_plan, segments):
    sent = pack(queries, key_proj, value_proj, out_grad, row_plan, segments)
    here = lax.all_to_all(
        sent.reshape(TOK, IN_ROWS, HEAD_DIM), ("dp", "ctx"), split_axis=0, concat_axis=0, tiled=True
    ).reshape(4, 32, IN_ROWS, HEAD_DIM)
    other = to_other_core(here[:, :, 64:96, :])
    rows, keep, give = attention(here, other)
    done = join(rows, keep, to_other_core(give))
    back = lax.all_to_all(
        done.reshape(TOK, OUT_ROWS, HEAD_DIM), ("dp", "ctx"), split_axis=0, concat_axis=0, tiled=True
    )
    return tuple(unpack(back.reshape(2, 2, 2, 16, OUT_ROWS, HEAD_DIM), row_plan))


def solution(mesh):
    rows = P(("dp", "ctx"), None)
    return jax.shard_map(
        on_device,
        mesh=mesh,
        in_specs=(rows, rows, rows, rows, P(("dp", "ctx")), P("dp", "ctx")),
        out_specs=(rows, rows, rows, rows),
        check_vma=False,
    )
```
